256 devices in a mesh: row: 32 (over x, z_hi, y), col: 8 (over z_lo, core).
Axes of the slice: x: 4, y: 4, z: 8 (z_hi: 2, z_lo: 4; z = z_hi * 4 + z_lo), core: 2. Of those that a mesh axis runs over, the one named last changes fastest.
Arguments:
- lanczos_now: float32 [1, 256, 1024], P(None, 'row', 'col'), may hold values from -80 to 80, as said below
- lanczos_prev: float32 [1, 256, 1024], P(None, 'row', 'col'), may hold values from -6 to 6
- beta_prev: float32 [1], replicated, may hold values from 0.3 to 1.5
- valence_energy: float32 [256], P('row'), may hold values from -1.5 to -0.5
- conduction_energy: float32 [1024], P('col'), may hold values from 0.5 to 2.5
- valence_panel: float32 [16384, 256], P(('row', 'col')), may hold values from -0.375 to 0.375
- conduction_panel: float32 [16384, 1024], P(('row', 'col')), may hold values from -0.1875 to 0.1875
- screened_coulomb: float32 [16384, 16384], P('row', 'col'), may hold values from -0.046875 to 0.046875
- bare_coulomb: float32 [16384, 16384], P('row', 'col'), may hold values from -0.046875 to 0.046875
Outputs:
- lanczos_next: float32 [1, 256, 1024], P(None, 'row', 'col')
- coefficients: float32 [1, 2], replicated
The draws below stay inside these ranges and needn't reach their ends.
Inputs may be any that keep to these rules, and one draw needn't show every extreme that they name: `lanczos_now`: real entries; the vectors of a chain are not normalized.
All inputs are finite; a program needn't handle non-finite values.
Results may differ from the reference program's by a relative error of at most 0.0002.
Values sent between devices are 32-bit elements; how exact they have to be, the bound alone decides.
A program may use at most 128 MiB of HBM per device.

```python
import math
import jax
import jax.numpy as jnp
from jax import lax

V = 256
C = 1024
NP = 16384
NVEC = 1


def draw_lanczos_now(key, part):
    noise_key, column_key = jax.random.split(key, 2)
    base = jnp.clip(jax.random.normal(noise_key, (NVEC, V, C), jnp.float32), -6.0, 6.0)
    position = jnp.arange(V, dtype=jnp.float32) / (V - 1)
    row_scale = 10.0 ** (position - 0.5)
    column_scale = jnp.exp(jax.random.uniform(column_key, (C,), jnp.float32, 0.0, math.log(3.0)))
    return base * row_scale[None, :, None] * column_scale[None, None, :]


def block_levels(key, dims, pieces, low, top_value):
    def one(axis_at, parts):
        steps = jax.random.uniform(jax.random.fold_in(jax.random.fold_in(key, 6), axis_at), (parts,), jnp.float32, low / len(pieces), top_value / len(pieces))
        return jnp.repeat(jnp.exp(steps), dims[axis_at] // parts).reshape((-1,) + (1,) * (len(dims) - axis_at - 1))

    factor_of = one(*pieces[0])
    for cut in pieces[1:]:
        factor_of = factor_of * one(*cut)
    return factor_of


def normal_values(stream_key, extent, width, limit, shards=(), kind=jnp.bfloat16):
    loudness = block_levels(stream_key, extent, shards, -0.22, 0.18) if shards else 1.0
    entries = jax.random.normal(stream_key, extent, jnp.float32) * width * loudness
    return jnp.minimum(jnp.maximum(entries, -limit), limit).astype(kind)


def setup_inputs(seed: int = 0) -> dict:
    key_of = jax.random.split(jax.random.key(seed), 10)
    return {
        "lanczos_now": draw_lanczos_now(jax.random.fold_in(key_of[9], 71), 0),
        "lanczos_prev": normal_values(key_of[1], (NVEC, V, C), 1.0, 6.0, ((1, 32), (2, 8)), jnp.float32),
        "beta_prev": jnp.clip(jnp.exp(jax.random.uniform(key_of[2], (NVEC,), jnp.float32, math.log(0.3), math.log(1.5))), 0.3, 1.5),
        "valence_energy": jnp.clip(-1.5 + 1.0 * jax.random.uniform(key_of[3], (V,), jnp.float32) ** block_levels(key_of[3], (V,), ((0, 32),), -0.2, 0.2), -1.5, -0.5),
        "conduction_energy": jnp.clip(0.5 + 2.0 * jax.random.uniform(key_of[4], (C,), jnp.float32) ** block_levels(key_of[4], (C,), ((0, 8),), -0.2, 0.2), 0.5, 2.5),
        "valence_panel": normal_values(key_of[5], (NP, V), V ** -0.5, 0.375, ((0, 256),), jnp.float32),
        "conduction_panel": normal_values(key_of[6], (NP, C), C ** -0.5, 0.1875, ((0, 256),), jnp.float32),
        "screened_coulomb": normal_values(key_of[7], (NP, NP), NP ** -0.5, 0.046875, ((0, 32), (1, 8)), jnp.float32),
        "bare_coulomb": normal_values(key_of[8], (NP, NP), NP ** -0.5, 0.046875, ((0, 32), (1, 8)), jnp.float32),
    }


precise = lax.Precision.HIGHEST
epsilon = 1e-06

def reference(lanczos_now, lanczos_prev, beta_prev, valence_energy, conduction_energy, valence_panel, conduction_panel, screened_coulomb, bare_coulomb):
    products = jnp.einsum('nv,kvc->knc', valence_panel, lanczos_now, precision=precise)
    density = lax.optimization_barrier(jnp.sum(products * conduction_panel[None], axis=2))
    potential = jnp.einsum('mn,kn->km', bare_coulomb, density, precision=precise)
    weighted = potential[:, :, None] * conduction_panel[None]
    exchange = jnp.einsum('mv,kmc->kvc', valence_panel, weighted, precision=precise)
    pair_amp = jnp.einsum('mc,kvc->kmv', conduction_panel, lanczos_now, precision=precise)
    block_size = min(512, NP)
    block_count = NP // block_size

    def one_block(index, total):
        first_row = (index * block_size).astype(jnp.int32)
        pair_rows = lax.dynamic_slice_in_dim(pair_amp, first_row, block_size, 1)
        kernel_rows = lax.dynamic_slice_in_dim(screened_coulomb, first_row, block_size, 0)
        cond_rows = lax.dynamic_slice_in_dim(conduction_panel, first_row, block_size, 0)
        pair_terms = jnp.einsum('kmv,nv->kmn', pair_rows, valence_panel, precision=precise) * kernel_rows[None]
        screened = jnp.einsum('kmn,nv->kmv', pair_terms, valence_panel, precision=precise)
        return total + jnp.einsum('kmv,mc->kvc', screened, cond_rows, precision=precise)
    direct = lax.fori_loop(0, block_count, one_block, jnp.zeros((NVEC, V, C), jnp.float32))
    gaps = conduction_energy[None, None, :] - valence_energy[None, :, None]
    image = gaps * lanczos_now + 2.0 * exchange - direct
    coef_alpha = lax.optimization_barrier(jnp.mean(lanczos_now * image, axis=(1, 2))) / (lax.optimization_barrier(jnp.mean(lanczos_now * lanczos_now, axis=(1, 2))) + epsilon)
    resid = image - coef_alpha[:, None, None] * lanczos_now - beta_prev[:, None, None] * lanczos_prev
    beta_next = jnp.sqrt(lax.optimization_barrier(jnp.mean(resid * resid, axis=(1, 2))) + epsilon)
    return (resid / beta_next[:, None, None], jnp.stack([coef_alpha, beta_next], axis=1))
```

```python
import functools

import jax
import jax.numpy as jnp
from jax import lax
from jax.experimental import pallas as pl
from jax.experimental.pallas import tpu as pltpu
from jax.sharding import PartitionSpec as P

MESH = pl.DeviceIdType.MESH
HIGHEST = lax.Precision.HIGHEST
V, C = 256, 1024
EPS = 1e-06
NN = (((1,), (0,)), ((), ()))
NT = (((1,), (1,)), ((), ()))
TN = (((0,), (0,)), ((), ()))


def halves(a):
    hi = a.astype(jnp.bfloat16)
    return hi, (a - hi.astype(jnp.float32)).astype(jnp.bfloat16)


def dot3(a, b, dims):
    d = functools.partial(lax.dot_general, dimension_numbers=dims, preferred_element_type=jnp.float32)
    return d(a[0], b[0]) + (d(a[0], b[1]) + d(a[1], b[0]))


def exact(a, b, dims):
    return lax.dot_general(a, b, dims, precision=HIGHEST, preferred_element_type=jnp.float32)


def kernel(
    q_ref, prev_ref, beta_ref, ev_ref, ec_ref, pv_hbm, pc_hbm, w_hbm, b_hbm,
    out_ref, coef_ref,
    w_ref, b_ref, pc_ref, xg, pst, pvc, ar, dst_, dc, sx, s0, s1, kb, r0, r1a, r1b, acc1a, acc1b, r2, acc2, r3,
    mine, tz, mid, txy,
    load_sem, x1s, x1r, x2s, x2r, x3s, x3r, x4s, x4r, p1s, p1r, p2s, p2r, p3s, p3r,
    as_, ar_sem, afs, afr, d1s, d1r, d2s, d2r, d3s, d3r, s0s, s0r, s1s, s1r,
    f0s, f0r, f1s, f1r, f2s, f2r, f3s, f3r, tzs, tzr, txs, txr,
):
    row, col = lax.axis_index("row"), lax.axis_index("col")
    x, zhi, y = row // 8, (row // 4) % 2, row % 4
    zlo, core = col // 2, col % 2
    z = zhi * 4 + zlo
    other = 1 - core

    def dev(px, py, pz, pcore):
        return (px * 8 + (pz // 4) * 4 + py, (pz % 4) * 2 + pcore)

    def rc(src, dst, ss, rs, to):
        return pltpu.make_async_remote_copy(
            src_ref=src, dst_ref=dst, send_sem=ss, recv_sem=rs, device_id=to, device_id_type=MESH
        )

    def px(d):
        return (x + d) % 4

    def py(d):
        return (y + d) % 4

    def pz(d):
        return (z + d) % 8

    partner = dev(x, y, z, other)
    me = dev(x, y, z, core)

    loads = [
        pltpu.make_async_copy(pv_hbm, pst.at[x], load_sem.at[0]),
        pltpu.make_async_copy(pc_hbm, pc_ref, load_sem.at[1]),
        pltpu.make_async_copy(w_hbm, w_ref, load_sem.at[2]),
        pltpu.make_async_copy(b_hbm, b_ref, load_sem.at[3]),
    ]
    for c in loads:
        c.start()

    barrier = pltpu.get_barrier_semaphore()

    def greet(to):
        pl.semaphore_signal(barrier, inc=1, device_id=to, device_id_type=MESH)

    greet(partner)
    for d in range(1, 8):
        greet(dev(x, y, pz(d), core))
        greet(dev(x, y, pz(d), other))
    for d in range(1, 16):
        greet(dev(px(d // 4), py(d % 4), z, core))
    xg[core, x, zhi, y, zlo] = q_ref[0]
    pl.semaphore_wait(barrier, 30)

    def x1(d):
        return rc(q_ref.at[0], xg.at[core, x, zhi, y, zlo], x1s.at[d], x1r.at[d], dev(x, y, pz(d), core))

    for d in range(1, 8):
        x1(d).start()
    loads[0].wait()

    def p1(d):
        return rc(pst.at[x], pst.at[x], p1s.at[d], p1r.at[d], dev(px(d), y, z, core))

    for d in range(1, 4):
        p1(d).start()
    for d in range(1, 8):
        x1(d).wait_recv()

    def x2(d):
        to = dev(jnp.where(core == 0, x, px(d)), jnp.where(core == 0, py(d), y), z, core)
        return rc(xg.at[core, x, :, y], xg.at[core, x, :, y], x2s.at[d], x2r.at[d], to)

    for d in range(1, 4):
        x2(d).start()

    def p2(d, h):
        k = px(-d + 4)
        return rc(
            pst.at[k], pvc.at[y, zlo, core], p2s.at[d * 2 + h], p2r.at[zlo * 2 + core], dev(x, y, k + 4 * h, zhi)
        )

    def p2_self(d, h):
        return (zhi == h) & (px(-d + 4) == zlo) & (core == zhi)

    for d in range(4):
        if d:
            p1(d).wait_recv()
        for h in range(2):

            @pl.when(p2_self(d, h))
            def _():
                pvc[y, zlo, core] = pst[zlo]

            @pl.when(jnp.logical_not(p2_self(d, h)))
            def _():
                p2(d, h).start()

    for d in range(1, 4):
        x2(d).wait_recv()

    def x3a(d):
        return rc(xg.at[core, x], xg.at[core, x], x3s.at[d], x3r.at[d], dev(px(d), y, z, core))

    def x3b(d):
        return rc(xg.at[core, :, :, y], xg.at[core, :, :, y], x3s.at[d], x3r.at[d], dev(x, py(d), z, core))

    def x4a(d):
        part = xg.at[core, px(4 - d)]
        return rc(part, part, x4s.at[d], x4r.at[d], partner)

    def x4b(d):
        part = xg.at[core, :, :, py(4 - d)]
        return rc(part, part, x4s.at[d], x4r.at[d], partner)

    @pl.when(core == 0)
    def _():
        for d in (2, 1, 3):
            x3a(d).start()
        x4a(0).start()

    @pl.when(core == 1)
    def _():
        for d in (2, 1, 3):
            x3b(d).start()
        x4b(0).start()

    for i in range(8):
        own = (i == zlo * 2 + core) & (zhi == core)

        @pl.when(jnp.logical_not(own))
        def _():
            rc(pst.at[0], pvc.at[y, i // 2, i % 2], p2s.at[0], p2r.at[i], partner).wait_recv()

    def p3(up, zl):
        to = dev(x, py(1 if up else 3), z, core)
        j = zl + (0 if up else 4)
        return rc(pvc.at[y, zl], pvc.at[y, zl], p3s.at[j], p3r.at[j], to)

    def p4(up, zl):
        yy = py(3 if up else 1)
        to = dev(x, py(1 if up else 3), z, core)
        j = 8 + zl
        return rc(pvc.at[yy, zl], pvc.at[yy, zl], p3s.at[j], p3r.at[j], to)

    for up, zl in ((1, 0), (0, 2), (1, 1), (0, 3), (1, 2), (0, 0), (1, 3), (0, 1)):
        p3(up, zl).start()

    @pl.when(core == 0)
    def _():
        for d in (1, 3, 2):
            x3a(d).wait_recv()
            x4a(d).start()

    @pl.when(core == 1)
    def _():
        for d in (1, 3, 2):
            x3b(d).wait_recv()
            x4b(d).start()

    for d in range(4):

        @pl.when(core == 0)
        def _():
            part = xg.at[1, :, :, py(4 - d)]
            rc(part, part, x4s.at[d], x4r.at[d], partner).wait_recv()

        @pl.when(core == 1)
        def _():
            part = xg.at[0, px(4 - d)]
            rc(part, part, x4s.at[d], x4r.at[d], partner).wait_recv()

    loads[1].wait()
    xfull = jnp.concatenate([xg[c % 2, :, :, :, c // 2].reshape(V, 128) for c in range(8)], axis=1)
    amp = exact(pc_ref[...], xfull, NT)
    ar[zlo, core] = amp

    def a1(d):
        to = (row, ((zlo + d) % 4) * 2 + core)
        return rc(ar.at[zlo, core], ar.at[zlo, core], as_.at[d], ar_sem.at[d], to)

    def a2(d):
        part = ar.at[(zlo + 4 - d) % 4, core]
        return rc(part, part, afs.at[d], afr.at[d], partner)

    for d in range(1, 4):
        a1(d).start()
    a2(0).start()
    dens = exact(jnp.ones((8, V), jnp.float32), pst[x] * amp, NT)
    dens = jnp.concatenate([dens, dens], axis=1)
    lane8 = lax.broadcasted_iota(jnp.int32, (8, 128), 1)
    dst_[x] = jnp.where(lane8 // 64 == core, dens, 0.0)

    def d1(d):
        return rc(dst_.at[x], dst_.at[x], d1s.at[d], d1r.at[d], dev(px(d), y, z, core))

    for d in range(1, 4):
        d1(d).start()

    def d2(d, h):
        k = px(-d + 4)
        return rc(
            dst_.at[k], dc.at[y, zlo, core], d2s.at[d * 2 + h], d2r.at[zlo * 2 + core], dev(x, y, k + 4 * h, zhi)
        )

    for d in range(4):
        if d:
            d1(d).wait_recv()
        for h in range(2):

            @pl.when(p2_self(d, h))
            def _():
                dc[y, zlo, core] = dst_[zlo]

            @pl.when(jnp.logical_not(p2_self(d, h)))
            def _():
                d2(d, h).start()

    for up, zl in ((1, 0), (0, 2), (1, 1), (0, 3)):
        j = zl + (0 if up else 4)
        yy = py(3 if up else 1)
        rc(pvc.at[yy, zl], pvc.at[yy, zl], p3s.at[j], p3r.at[j], partner).wait_recv()
        p4(up, zl).start()

    for d in range(1, 4):
        part = ar.at[(zlo + 4 - d) % 4, core]
        rc(part, part, as_.at[d], ar_sem.at[d], partner).wait_recv()
        a2(d).start()
    for i in range(8):
        own = (i == zlo * 2 + core) & (zhi == core)

        @pl.when(jnp.logical_not(own))
        def _():
            rc(dst_.at[0], dc.at[y, i // 2, i % 2], d2s.at[0], d2r.at[i], partner).wait_recv()

    def d3(d):
        return rc(dc.at[y], dc.at[y], d3s.at[d], d3r.at[d], dev(x, py(d), z, core))

    for d in range(1, 4):
        d3(d).start()
    for d in range(4):
        part = ar.at[(zlo + 4 - d) % 4, other]
        rc(part, part, afs.at[d], afr.at[d], partner).wait_recv()

    loads[2].wait()
    amps = halves(ar[...].reshape(512, V))
    total = None
    for g in range(4):
        yy = py((0, 3, 1, 2)[g])
        if g == 1:
            for zl in (2, 3):
                rc(pvc.at[yy, zl], pvc.at[yy, zl], p3s.at[0], p3r.at[zl], partner).wait_recv()
        if g == 2:
            for zl in (0, 1):
                rc(pvc.at[yy, zl], pvc.at[yy, zl], p3s.at[0], p3r.at[4 + zl], partner).wait_recv()
        if g == 3:
            for zl in range(4):
                rc(pvc.at[yy, zl], pvc.at[yy, zl], p3s.at[0], p3r.at[8 + zl], partner).wait_recv()
        panel = halves(pvc[yy].reshape(512, V))
        at = pl.ds(pl.multiple_of(yy * 512, 512), 512)
        terms = dot3(amps, panel, NT) * w_ref[:, at]
        part = dot3(halves(terms), panel, NN)
        total = part if total is None else total + part

    sx[:, :, 0:64, :] = total.reshape(4, 2, 64, V)

    for d in range(1, 4):
        part = dc.at[py(4 - d)]
        rc(part, part, d3s.at[d], d3r.at[d], partner).wait_recv()
    loads[3].wait()
    dens_row = dc[:, :, 0, 0:1, :] + dc[:, :, 1, 0:1, :]
    pot = None
    for t in range(16):
        piece = b_ref[:, t * 128 : (t + 1) * 128] * dens_row[t // 4, t % 4]
        pot = piece if pot is None else pot + piece
    pot = jnp.sum(pot, axis=1, keepdims=True)
    sub = lax.broadcasted_iota(jnp.int32, (64, 128), 0)
    lane = lax.broadcasted_iota(jnp.int32, (64, 128), 1)
    diag = sub == lane
    for j in range(8):
        line = jnp.sum(jnp.where(diag, pot[j * 64 : (j + 1) * 64], 0.0), axis=0, keepdims=True)
        line = jnp.concatenate([jnp.broadcast_to(line, (8, 128)), jnp.zeros((8, 128), jnp.float32)], axis=1)
        sx[j // 2, j % 2, 64:72, :] = line

    def sa(zl):
        return rc(sx.at[zl, other], s0.at[zl], s0s.at[zl], s0r.at[zl], partner)

    def sb(d):
        zl = (zlo + d) % 4
        return rc(sx.at[zl, core], s1.at[d], s1s.at[d], s1r.at[d], (row, zl * 2 + core))

    order = [(zlo + d) % 4 for d in (2, 1, 3, 0)]
    for zl in order:
        sa(zl).start()
    for d, zl in zip((2, 1, 3, 0), order):
        sa(zl).wait_recv()
        sx[zl, core] = sx[zl, core] + s0[zl]
        if d:
            sb(d).start()
    for d in range(1, 4):
        sb(d).wait_recv()
    mine_s = sx[zlo, core] + s1[1] + s1[2] + s1[3]

    pot_row = mine_s[64:65, 0:128]
    pot_col = jnp.sum(jnp.where(diag, pot_row, 0.0), axis=1, keepdims=True)
    both = 2.0 * pot_col * pst[x] - mine_s[0:64]
    kpart = exact(both, pc_ref[...], TN)
    for c in range(8):
        kb[c % 2, :, :, :, c // 2] = kpart[:, c * 128 : (c + 1) * 128].reshape(4, 2, 4, 8, 128)

    def f0(i):
        return rc(kb.at[other, i], r0.at[i], f0s.at[i], f0r.at[i], partner)

    for i in range(4):
        f0(i).start()
    for i in range(4):
        f0(i).wait_recv()
        kb[core, i] = kb[core, i] + r0[i]

    def f1a(d):
        return rc(kb.at[core, px(d)], r1a.at[d - 1], f1s.at[d], f1r.at[d], dev(px(d), y, z, core))

    def f1b(d):
        return rc(kb.at[core, :, :, py(d)], r1b.at[d - 1], f1s.at[d], f1r.at[d], dev(x, py(d), z, core))

    def f2a(d):
        return rc(acc1a.at[:, py(d)], r2.at[d - 1], f2s.at[d], f2r.at[d], dev(x, py(d), z, core))

    def f2b(d):
        return rc(acc1b.at[px(d)], r2.at[d - 1], f2s.at[d], f2r.at[d], dev(px(d), y, z, core))

    @pl.when(core == 0)
    def _():
        for d in (2, 1, 3):
            f1a(d).start()
        for d in range(1, 4):
            f1a(d).wait_recv()
        acc1a[...] = kb[0, x] + r1a[0] + r1a[1] + r1a[2]
        for d in (2, 1, 3):
            f2a(d).start()
        for d in range(1, 4):
            f2a(d).wait_recv()
        acc2[...] = acc1a[:, y] + r2[0] + r2[1] + r2[2]

    @pl.when(core == 1)
    def _():
        for d in (2, 1, 3):
            f1b(d).start()
        for d in range(1, 4):
            f1b(d).wait_recv()
        acc1b[...] = kb[1, :, :, y] + r1b[0] + r1b[1] + r1b[2]
        for d in (2, 1, 3):
            f2b(d).start()
        for d in range(1, 4):
            f2b(d).wait_recv()
        acc2[...] = acc1b[x] + r2[0] + r2[1] + r2[2]

    def f3(d):
        zz = pz(d)
        return rc(acc2.at[zz // 4, zz % 4], r3.at[d], f3s.at[d], f3r.at[d], dev(x, y, zz, core))

    for d in range(1, 8):
        f3(d).start()
    for d in range(1, 8):
        f3(d).wait_recv()
    tile = acc2[zhi, zlo]
    for d in range(1, 8):
        tile = tile + r3[d]

    q, prev = q_ref[0], prev_ref[0]
    sub8 = lax.broadcasted_iota(jnp.int32, (8, 128), 0)
    ev = jnp.zeros((8, 128), jnp.float32)
    for i in range(8):
        ev = jnp.where(sub8 == i, ev_ref[i], ev)
    ec = ec_ref[...].reshape(1, 128)
    image = (ec - ev) * q + tile
    sums = jnp.zeros((8, 128), jnp.float32)
    for i, term in enumerate((q * image, q * q, image * image, image * prev, prev * prev, q * prev)):
        sums = jnp.where(sub8 == i, jnp.sum(term, axis=0, keepdims=True), sums)
    mine[...] = sums

    def t1(j):
        d, c = j % 8, j // 8
        return rc(mine, tz.at[j], tzs.at[j], tzr.at[j], dev(x, y, pz(d), core if c == 0 else other))

    for j in range(1, 16):
        t1(j).start()
    for j in range(1, 16):
        t1(j).wait_recv()
    part = sums
    for j in range(1, 16):
        part = part + tz[j]
    mid[...] = part

    def t2(j):
        return rc(mid, txy.at[j], txs.at[j], txr.at[j], dev(px(j // 4), py(j % 4), z, core))

    for j in range(1, 16):
        t2(j).start()
    for j in range(1, 16):
        t2(j).wait_recv()
    for j in range(1, 16):
        part = part + txy[j]
    part = jnp.sum(part, axis=1, keepdims=True)
    qu, qq, uu, up_, pp, qp = (part[i : i + 1] for i in range(6))
    inv = 1.0 / (V * C)
    bp = beta_ref[0]
    alpha = qu * inv / (qq * inv + EPS)
    ww = (
        uu - 2.0 * alpha * qu - 2.0 * bp * up_ + alpha * alpha * qq + bp * bp * pp + 2.0 * alpha * bp * qp
    ) * inv
    beta = jnp.sqrt(ww + EPS)
    out_ref[0] = (image - alpha * q - bp * prev) / beta
    two = lax.broadcasted_iota(jnp.int32, (1, 2), 1)
    coef_ref[...] = jnp.where(two == 0, alpha, beta)

    for d in range(1, 8):
        x1(d).wait_send()
        f3(d).wait_send()
    for d in range(1, 4):
        x2(d).wait_send()
        p1(d).wait_send()
        a1(d).wait_send()
        d1(d).wait_send()
        d3(d).wait_send()
        sb(d).wait_send()
    for d in range(4):
        a2(d).wait_send()
        f0(d).wait_send()
        sa(d).wait_send()
        for h in range(2):

            @pl.when(jnp.logical_not(p2_self(d, h)))
            def _():
                p2(d, h).wait_send()
                d2(d, h).wait_send()

    for zl in range(4):
        p3(1, zl).wait_send()
        p3(0, zl).wait_send()
        p4(1 if zl < 2 else 0, zl).wait_send()

    @pl.when(core == 0)
    def _():
        for d in range(4):
            x4a(d).wait_send()
            if d:
                x3a(d).wait_send()
                f1a(d).wait_send()
                f2a(d).wait_send()

    @pl.when(core == 1)
    def _():
        for d in range(4):
            x4b(d).wait_send()
            if d:
                x3b(d).wait_send()
                f1b(d).wait_send()
                f2b(d).wait_send()

    for j in range(1, 16):
        t1(j).wait_send()
        t2(j).wait_send()


def per_device(q, prev, beta, ev, ec, pv, pc, w, b):
    f32 = jnp.float32
    vmem = pl.BlockSpec(memory_space=pltpu.VMEM)
    smem = pl.BlockSpec(memory_space=pltpu.SMEM)
    hbm = pl.BlockSpec(memory_space=pl.ANY)

    def buf(*shape):
        return pltpu.VMEM(shape, f32)

    def sem(n):
        return pltpu.SemaphoreType.DMA((n,))

    tile = (8, 128)
    scratch = [
        buf(512, 2048), buf(512, 2048), buf(64, C),
        buf(2, 4, 2, 4, 4, *tile),
        buf(4, 64, V), buf(4, 4, 2, 64, V),
        buf(4, 2, 64, V),
        buf(4, *tile), buf(4, 4, 2, *tile),
        buf(4, 2, 72, V), buf(4, 72, V), buf(4, 72, V),
        buf(2, 4, 2, 4, 4, *tile), buf(4, 2, 4, 4, *tile),
        buf(3, 2, 4, 4, *tile), buf(3, 4, 2, 4, *tile),
        buf(2, 4, 4, *tile), buf(4, 2, 4, *tile),
        buf(3, 2, 4, *tile), buf(2, 4, *tile), buf(8, *tile),
        buf(*tile), buf(16, *tile), buf(*tile), buf(16, *tile),
        sem(4),
        sem(8), sem(8), sem(4), sem(4), sem(4), sem(4), sem(4), sem(4),
        sem(4), sem(4), sem(8), sem(8), sem(12), sem(12),
        sem(4), sem(4), sem(4), sem(4),
        sem(4), sem(4), sem(8), sem(8), sem(4), sem(4),
        sem(4), sem(4), sem(4), sem(4),
        sem(4), sem(4), sem(4), sem(4), sem(4), sem(4), sem(8), sem(8),
        sem(16), sem(16), sem(16), sem(16),
    ]
    return pl.pallas_call(
        kernel,
        out_shape=(jax.ShapeDtypeStruct((1, 8, 128), f32), jax.ShapeDtypeStruct((1, 2), f32)),
        in_specs=[vmem, vmem, smem, smem, vmem, hbm, hbm, hbm, hbm],
        out_specs=(vmem, vmem),
        scratch_shapes=scratch,
        compiler_params=pltpu.CompilerParams(
            collective_id=0, has_side_effects=True, vmem_limit_bytes=60 * 1024 * 1024
        ),
        name="lanczos_step",
    )(q, prev, beta, ev, ec, pv, pc, w, b)


def solution(mesh):
    return jax.shard_map(
        per_device,
        mesh=mesh,
        in_specs=(
            P(None, "row", "col"),
            P(None, "row", "col"),
            P(),
            P("row"),
            P("col"),
            P(("row", "col"), None),
            P(("row", "col"), None),
            P("row", "col"),
            P("row", "col"),
        ),
        out_specs=(P(None, "row", "col"), P()),
        check_vma=False,
    )
```

```python
import functools

import jax
import jax.numpy as jnp
from jax import lax
from jax.experimental import pallas as pl
from jax.experimental.pallas import tpu as pltpu
from jax.sharding import PartitionSpec as P

MESH = pl.DeviceIdType.MESH
HIGHEST = lax.Precision.HIGHEST
V, C = 256, 1024
EPS = 1e-06
NN = (((1,), (0,)), ((), ()))
NT = (((1,), (1,)), ((), ()))
TN = (((0,), (0,)), ((), ()))


def halves(a):
    hi = a.astype(jnp.bfloat16)
    return hi, (a - hi.astype(jnp.float32)).astype(jnp.bfloat16)


def left3(a, axis):
    hi, lo = halves(a)
    return jnp.concatenate([hi, lo, hi], axis=axis)


def right3(a, axis):
    hi, lo = halves(a)
    return jnp.concatenate([hi, hi, lo], axis=axis)


def dot(a, b, dims):
    return lax.dot_general(a, b, dims, preferred_element_type=jnp.float32)


def exact(a, b, dims):
    return lax.dot_general(a, b, dims, precision=HIGHEST, preferred_element_type=jnp.float32)


def kernel(
    beta_hbm, ev_hbm, q_hbm, prev_hbm, ec_hbm, pv_hbm, pc_hbm, w_hbm, b_hbm,
    out_ref, coef_ref,
    beta_ref, ev_ref, ec_ref, q_ref, prev_ref, own_pv, pc_other, w_ref, b_ref, pcr, pch, pcl, pvr, xg, pvc, ph, pl_,
    ap, ao, asum, amps, dmine, dc, potx, pot0, ee, eo, dd, kb, r1a, r1b, acc1, r3,
    tz, txy, az, axy, mid, amid, dummy,
    load_sem, send_sem,
    x1r, x2r, x3r, p2r, p3r, p4r, p5r, cr, vr, v2r, ar_, dr, q0r, er, f1r, f3r, tr,
):
    row, col = lax.axis_index("row"), lax.axis_index("col")
    x, zhi, y = row // 8, (row // 4) % 2, row % 4
    zlo, core = col // 2, col % 2
    z = zhi * 4 + zlo
    other = 1 - core
    a, b = jnp.where(core == 0, y, x), jnp.where(core == 0, x, y)

    def dev(px, py, pz, pcore):
        return (px * 8 + (pz // 4) * 4 + py, (pz % 4) * 2 + pcore)

    def rc(src, dst, group, rs, to):
        return pltpu.make_async_remote_copy(
            src_ref=src, dst_ref=dst, send_sem=send_sem.at[group], recv_sem=rs, device_id=to, device_id_type=MESH
        )

    def px(d):
        return (x + d) % 4

    def py(d):
        return (y + d) % 4

    def pz(d):
        return (z + d) % 8

    def ab(da, db, dz=0):
        ja, jb = (a + da) % 4, (b + db) % 4
        return dev(jnp.where(core == 0, jb, ja), jnp.where(core == 0, ja, jb), pz(dz), core)

    partner = dev(x, y, z, other)

    def arrived(rs, kib):
        part = dummy.at[pl.ds(0, kib * 2)]
        rc(part, part, 0, rs, partner).wait_recv()

    def left(group, kib):
        part = dummy.at[pl.ds(0, kib * 2)]
        rc(part, part, group, x1r, partner).wait_send()

    def rows_arrived(rs, ref, n):
        part = ref.at[pl.ds(0, n)]
        rc(part, part, 0, rs, partner).wait_recv()

    def rows_left(group, ref, n):
        part = ref.at[pl.ds(0, n)]
        rc(part, part, group, x1r, partner).wait_send()

    lanes = [slice(c * 128, (c + 1) * 128) for c in range(4)]
    pairs = [(q_hbm, q_ref), (pv_hbm, own_pv)]
    for c in range(4):
        mine, its = (pl.ds(pl.multiple_of((c * 2 + k) * 128, 128), 128) for k in (core, other))
        pairs.append((pc_hbm.at[:, mine], pcr.at[zlo, core, :, lanes[c]]))
        pairs.append((pc_hbm.at[:, its], pc_other.at[:, lanes[c]]))
    pairs += [(prev_hbm, prev_ref), (ec_hbm, ec_ref), (ev_hbm, ev_ref), (beta_hbm, beta_ref)]
    pairs += [(w_hbm, w_ref), (b_hbm, b_ref)]
    loads = [pltpu.make_async_copy(s, d, load_sem.at[i]) for i, (s, d) in enumerate(pairs)]
    for c in loads:
        c.start()

    barrier = pltpu.get_barrier_semaphore()

    def greet(to):
        pl.semaphore_signal(barrier, inc=1, device_id=to, device_id_type=MESH)

    in_own_block = (x == zlo) & (core == zhi)
    for i in range(8):
        to = dev(zlo, y, core * 4 + (zlo + i // 2) % 4, (core + i % 2) % 2)
        if i == 0:

            @pl.when(jnp.logical_not(in_own_block))
            def _():
                greet(to)

        else:
            greet(to)
    for d in range(1, 4):
        greet(dev(px(d), y, z, core))
        greet(dev(x, py(d), z, core))
    for d in (4, 3, 5, 2, 6, 1, 7):
        greet(dev(x, y, pz(d), core))
        greet(dev(x, y, pz(d), other))
    greet(partner)
    loads[0].wait()
    xg[x, zhi, y, zlo] = q_ref[0]
    for i in range(1, 10):
        loads[i].wait()
    pvr[zlo, core] = own_pv[...]

    @pl.when(in_own_block)
    def _():
        pvc[y, zlo * 2 + core, x] = own_pv[pl.ds(pl.multiple_of(x * 16, 16), 16)]
        pl.semaphore_wait(barrier, 21 + 7)

    @pl.when(jnp.logical_not(in_own_block))
    def _():
        pl.semaphore_wait(barrier, 21 + 8)

    for d in (4, 3, 5, 2, 6, 1, 7):
        rc(q_ref.at[0], xg.at[x, zhi, y, zlo], 0, x1r, dev(x, y, pz(d), core)).start()

    for i in range(8):
        quarter, to = px(i // 2), dev(px(i // 2), y, x + 4 * ((zhi + i % 2) % 2), zhi)
        part = own_pv.at[pl.ds(pl.multiple_of(quarter * 16, 16), 16)]
        copy = rc(part, pvc.at[y, zlo * 2 + core, quarter], 2, p2r, to)
        if i == 0:
            pl.when(jnp.logical_not(in_own_block))(copy.start)
        else:
            copy.start()

    def block_wait(wait, sem, per, n, *rest):
        @pl.when(in_own_block)
        def _():
            wait(sem, *rest, per * (n - 1))

        @pl.when(jnp.logical_not(in_own_block))
        def _():
            wait(sem, *rest, per * n)

    def inside(s):
        return (zlo + s >= 0) & (zlo + s < 4)

    own_rows = pcr.at[zlo, core]
    rc(pc_other, own_rows, 1, cr.at[0], partner).start()
    def rows_came(s):
        arrived(cr.at[s] if s > 0 else cr.at[3 - s], 256)

    arrived(x1r, 28)

    part = xg.at[x, :, y]
    for d in (2, 1, 3):
        rc(part, part, 0, x2r, ab(d, 0)).start()

    block_wait(arrived, p2r, 16, 8)
    def unit(da, db):
        ja, jb = (a + da) % 4, (b + db) % 4
        return pvc.at[jnp.where(core == 0, ja, jb), :, jnp.where(core == 0, jb, ja)]

    def p3(d):
        return rc(unit(0, 0), unit(0, 0), 5, p3r.at[d], ab(d, 0))

    def p4(up, rel):
        part = unit(rel, 0)
        return rc(part, part, 6, p4r.at[up * 4 + rel], ab(0, 1 if up else 3))

    def p4_came(up, rel):
        part = unit(rel, 3 if up else 1)
        rc(part, part, 6, p4r.at[up * 4 + rel], partner).wait_recv()

    def p5(up, rel):
        part = unit(rel, 3 if up else 1)
        return rc(part, part, 7, p5r, ab(0, 1 if up else 3))

    for d in (2, 1, 3):
        p3(d).start()
    for s in (2, -2, 1, -1):

        @pl.when(inside(s))
        def _():
            rc(own_rows, own_rows, 3, cr.at[abs(s)] if s > 0 else cr.at[3 + abs(s)], (row, (zlo + s) * 2 + core)).start()
            rc(pc_other, own_rows, 3, cr.at[abs(s)] if s > 0 else cr.at[3 + abs(s)], (row, (zlo + s) * 2 + other)).start()

    for s in (2, -2, 1, -1):

        @pl.when(inside(s))
        def _():
            rc(pvr.at[zlo, core], pvr.at[zlo, core], 4, vr.at[s + 3], (row, (zlo + s) * 2 + core)).start()

    arrived(x2r, 96)

    def chunk(c, d):
        return xg.at[px(d)] if c == 0 else xg.at[:, :, py(d)]

    for c in range(2):

        @pl.when(core == c)
        def _():
            for d in (2, 1, 3):
                rc(chunk(c, 0), chunk(c, 0), 8, x3r, ab(0, d)).start()

    p4(1, 0).start()
    p4(0, 0).start()

    for d in (1, 3, 2):
        part = unit(4 - d, 0)
        rc(part, part, 5, p3r.at[d], partner).wait_recv()
        p4(1, 4 - d).start()
        p4(0, 4 - d).start()

    arrived(x3r, 384)
    arrived(cr.at[0], 128)

    xs = left3(jnp.concatenate([xg[:, :, :, c].reshape(V, 128) for c in range(4)], axis=1), 1)

    def a1(zl):
        return rc(ap.at[zl], ao.at[zl], 10, ar_.at[zl], partner)

    def amp_of(zl):
        at = pl.ds(pl.multiple_of(zl * 128, 128), 128)
        hi, lo = halves(pcr[zl].reshape(128, 512))
        pch[at] = hi
        pcl[at] = lo
        ap[zl] = dot(jnp.concatenate([hi, hi, lo], axis=1), xs, NT).reshape(2, 64, V)
        a1(zl).start()

    amp_of(zlo)

    def relays(s):
        return inside(-s) & inside(s // 2)

    for s in (2, -2):

        @pl.when(relays(s))
        def _():
            rows_came(s)
            part = pcr.at[zlo - s]
            rc(part, part, 9, cr.at[3] if s > 0 else cr.at[6], (row, (zlo + s // 2) * 2 + core)).start()

    for up, rel in ((1, 0), (0, 3)):
        p4_came(up, rel)
        p5(up, rel).start()

    a1(zlo).wait_recv()
    own_amp = ap[zlo, core] + ao[zlo, core]
    dens = exact(jnp.ones((8, V), jnp.float32), own_pv[...] * own_amp, NT)[0:1]
    dens = jnp.concatenate([dens, dens], axis=1)
    lane1 = lax.broadcasted_iota(jnp.int32, (1, 128), 1)
    dmine[...] = jnp.where(lane1 // 64 == core, dens, 0.0)
    slot = y * 8 + zlo * 2 + core
    for i in range(32):
        to = dev(px(2 + i // 8), py(2 + (i // 2) % 4), x + 4 * ((zhi + i % 2) % 2), zhi)
        copy = rc(dmine, dc.at[slot], 11, dr, to)
        if i == 20:

            @pl.when(in_own_block)
            def _():
                dc[slot] = dmine[...]

            pl.when(jnp.logical_not(in_own_block))(copy.start)
        else:
            copy.start()

    for up, rel in ((1, 1), (0, 2)):
        p4_came(up, rel)
        p5(up, rel).start()

    for s in (2, -2):

        @pl.when(inside(-s) & jnp.logical_not(relays(s)))
        def _():
            rows_came(s)

        @pl.when(inside(-s))
        def _():
            amp_of(zlo - s)

    for s in (1, -1):

        @pl.when(inside(-s))
        def _():
            rows_came(s)
            amp_of(zlo - s)

    def v_came(s):
        part = pvr.at[zlo - s, core]
        rc(part, part, 4, vr.at[s + 3], partner).wait_recv()

    def v2(s):
        part = pvr.at[zlo - s, core]
        return rc(part, part, 14, v2r, partner)

    v2(0).start()
    for s in (2, -2, 1, -1):

        @pl.when(inside(-s))
        def _():
            v_came(s)
            v2(s).start()

        if abs(s) == 2:

            @pl.when(relays(s))
            def _():
                part = pvr.at[zlo - s, core]
                rc(part, part, 12, vr.at[s // 2 * 3 + 3], (row, (zlo + s // 2) * 2 + core)).start()

    for s in (3, -3):

        @pl.when(inside(-s))
        def _():
            rows_came(s)
            amp_of(zlo - s)

    for up, rel in ((1, 3), (1, 2), (0, 0), (0, 1)):
        p4_came(up, rel)
    arrived(p5r, 512)
    loads[14].wait()
    hi, lo = halves(pvc[...].reshape(2048, V))
    ph[...] = hi
    pl_[...] = lo
    for d in range(1, 4):
        a1((zlo + d) % 4).wait_recv()
    asum[...] = ap[...] + ao[...]
    amps[...] = left3(asum[...].reshape(512, V), 1)

    def block(g, rows):
        at = slice(g * 512, (g + 1) * 512)
        hi, lo = ph[at], pl_[at]
        terms = dot(amps[rows], jnp.concatenate([hi, hi, lo], axis=1), NT) * w_ref[rows, at]
        return dot(left3(terms, 1), jnp.concatenate([hi, hi, lo], axis=0), NN)

    def e1(i):
        part = pl.ds(2 * i, 2)
        return rc(ee.at[part], eo.at[part], 13, er.at[i], partner)

    def half(i):
        rows = slice(i * 256, (i + 1) * 256)
        part = block(0, rows) + block(1, rows) + block(2, rows) + block(3, rows)
        ee[2 * i : 2 * i + 2] = part.reshape(2, 2, 64, V)
        e1(i).start()

    half(0)

    loads[15].wait()
    block_wait(rows_arrived, dr, 1, 32, dc)
    pot = None
    for t in range(16):
        piece = b_ref[:, t * 128 : (t + 1) * 128] * (dc[2 * t] + dc[2 * t + 1])
        pot = piece if pot is None else pot + piece
    potx[...] = jnp.broadcast_to(jnp.sum(pot, axis=1, keepdims=True), (512, 128)).reshape(4, 2, 64, 128)

    def q0():
        return rc(potx, pot0, 15, q0r, partner)

    q0().start()
    half(1)

    for s in (3, -3):

        @pl.when(inside(-s))
        def _():
            v_came(s)
            v2(s).start()

    q0().wait_recv()
    arrived(v2r, 256)

    def kpart(i):
        e1(i).wait_recv()
        at = slice(2 * i, 2 * i + 2)
        pot2 = 2.0 * (potx[at] + pot0[at])
        both = jnp.concatenate([pot2, pot2], axis=3) * pvr[at] - (ee[at] + eo[at])
        dd[at] = both
        rows = slice(i * 256, (i + 1) * 256)
        hi, lo = pch[rows], pcl[rows]
        return dot(left3(both.reshape(256, V), 0), jnp.concatenate([hi, hi, lo], axis=0), TN)

    kfull = kpart(0)
    kfull = kfull + kpart(1)
    for c in range(4):
        kb[:, :, :, c] = kfull[:, lanes[c]].reshape(4, 2, 4, 8, 128)

    for c in range(2):

        @pl.when(core == c)
        def _():
            for d in (2, 1, 3):
                part = kb.at[px(d)] if c == 0 else kb.at[:, :, py(d)]
                rc(part, (r1a if c == 0 else r1b).at[d - 1], 16, f1r, ab(0, d)).start()

    for i in (10, 11, 12, 13):
        loads[i].wait()
    q, prev = q_ref[0], prev_ref[0]
    sub8 = lax.broadcasted_iota(jnp.int32, (8, 128), 0)
    ev = jnp.zeros((8, 128), jnp.float32)
    for i in range(8):
        ev = jnp.where(sub8 == i, ev_ref[i], ev)
    gaps = ec_ref[...].reshape(1, 128) - ev
    prod = (dd[:, core] * asum[:, core]).reshape(256, V)
    prod = jnp.sum(prod[:, 0:128] + prod[:, 128:256], axis=0, keepdims=True)
    qq = jnp.sum(q * q, axis=0, keepdims=True)
    qu = prod + jnp.sum(gaps * q * q, axis=0, keepdims=True)
    az[0] = jnp.concatenate([qu, qq], axis=1)

    def t1(src, dst, group, rs):
        for d in (4, 3, 5, 2, 6, 1, 7, 0):
            for j in (d, d + 8):
                if j:
                    to = dev(x, y, pz(d), core if j < 8 else other)
                    rc(src, dst.at[j], group, rs, to).start()

    def t2(src, dst, group, rs):
        for j in (10, 9, 11, 6, 14, 2, 8, 5, 7, 13, 15, 1, 3, 4, 12):
            rc(src, dst.at[j], group, rs, dev(px(j // 4), py(j % 4), z, core)).start()

    t1(az.at[0], az, 18, tr.at[0])

    arrived(f1r, 384)
    for c in range(2):

        @pl.when(core == c)
        def _():
            if c == 0:
                for i in range(2):
                    acc1[:, i] = kb[x, i] + r1a[0, i] + r1a[1, i] + r1a[2, i]
            else:
                acc1[...] = kb[:, :, y] + r1b[0] + r1b[1] + r1b[2]

    for da in (2, 1, 3, 0):
        for dz in (4, 3, 5, 2, 6, 1, 7, 0):
            if da or dz:
                zz = pz(dz)
                part = acc1.at[(a + da) % 4, zz // 4, zz % 4]
                rc(part, r3.at[da * 8 + dz], 17, f3r, ab(da, 0, dz)).start()
    rows_arrived(tr.at[0], az, 15)
    amid[...] = jnp.sum(az[...], axis=0)
    axy[0] = amid[...]
    t2(amid, axy, 19, tr.at[1])
    arrived(f3r, 124)
    tile = acc1[a, zhi, zlo] + jnp.sum(r3[1:32], axis=0)
    inv = 1.0 / (V * C)
    bp = beta_ref[0]
    rows_arrived(tr.at[1], axy, 15)
    total = jnp.sum(axy[...], axis=0)
    qu = jnp.sum(total[:, 0:128], axis=1, keepdims=True)
    qq = jnp.sum(total[:, 128:256], axis=1, keepdims=True)
    alpha = qu * inv / (qq * inv + EPS)
    resid = tile + (gaps - alpha) * q - bp * prev
    tz[0] = jnp.sum(resid * resid, axis=0, keepdims=True)
    t1(tz.at[0], tz, 20, tr.at[2])
    rows_arrived(tr.at[2], tz, 15)
    mid[...] = jnp.sum(tz[...], axis=0)
    t2(mid, txy, 21, tr.at[3])
    txy[0] = mid[...]
    rows_arrived(tr.at[3], txy, 15)
    ww = jnp.sum(jnp.sum(txy[...], axis=0), axis=1, keepdims=True)
    beta = jnp.sqrt(ww * inv + EPS)
    out_ref[0] = resid / beta
    two = lax.broadcasted_iota(jnp.int32, (1, 2), 1)
    coef_ref[...] = jnp.where(two == 0, alpha, beta)

    left(0, 124)
    left(1, 128)
    block_wait(left, 2, 16, 8)
    left(5, 384)
    left(6, 1024)
    left(7, 512)
    left(8, 384)

    @pl.when((zlo == 0) | (zlo == 3))
    def _():
        left(3, 512)
        left(4, 128)

    @pl.when((zlo == 1) | (zlo == 2))
    def _():
        left(3, 768)
        left(4, 192)
        left(9, 256)
        left(12, 64)

    left(10, 512)
    block_wait(rows_left, 11, 1, 32, dc)
    left(13, 512)
    left(14, 256)
    left(15, 256)
    left(16, 384)
    left(17, 124)
    rows_left(18, az, 15)
    rows_left(19, axy, 15)
    rows_left(20, tz, 15)
    rows_left(21, txy, 15)


def per_device(q, prev, beta, ev, ec, pv, pc, w, b):
    f32 = jnp.float32
    vmem = pl.BlockSpec(memory_space=pltpu.VMEM)
    hbm = pl.BlockSpec(memory_space=pl.ANY)

    def buf(*shape):
        return pltpu.VMEM(shape, f32)

    def sem(*n):
        return pltpu.SemaphoreType.DMA(n)

    tile = (8, 128)
    bf16 = jnp.bfloat16
    scratch = [
        pltpu.SMEM((1,), f32), pltpu.SMEM((8,), f32), buf(128),
        buf(1, *tile), buf(1, *tile), buf(64, V), buf(64, 512), buf(512, 2048), buf(512, 2048),
        buf(4, 2, 64, 512), pltpu.VMEM((512, 512), bf16), pltpu.VMEM((512, 512), bf16), buf(4, 2, 64, V),
        buf(4, 2, 4, 4, *tile), buf(4, 8, 4, 16, V), pltpu.VMEM((2048, V), bf16), pltpu.VMEM((2048, V), bf16),
        buf(4, 2, 64, V), buf(4, 2, 64, V), buf(4, 2, 64, V), pltpu.VMEM((512, 3 * V), bf16),
        buf(1, 128), buf(32, 1, 128), buf(4, 2, 64, 128), buf(4, 2, 64, 128),
        buf(4, 2, 64, V), buf(4, 2, 64, V), buf(4, 2, 64, V),
        buf(4, 2, 4, 4, *tile), buf(3, 2, 4, 4, *tile), buf(3, 4, 2, 4, *tile), buf(4, 2, 4, *tile), buf(32, *tile),
        buf(16, 1, 128), buf(16, 1, 128), buf(16, 1, 256), buf(16, 1, 256), buf(1, 128), buf(1, 256), buf(2048, 128),
        sem(16), sem(22),
        sem(), sem(), sem(), sem(), sem(4), sem(8), sem(), sem(7), sem(7), sem(), sem(4), sem(), sem(),
        sem(2), sem(), sem(), sem(4),
    ]
    return pl.pallas_call(
        kernel,
        out_shape=(jax.ShapeDtypeStruct((1, 8, 128), f32), jax.ShapeDtypeStruct((1, 2), f32)),
        in_specs=[hbm] * 9,
        out_specs=(vmem, vmem),
        scratch_shapes=scratch,
        compiler_params=pltpu.CompilerParams(
            collective_id=0, has_side_effects=True, vmem_limit_bytes=60 * 1024 * 1024
        ),
        name="lanczos_step",
    )(beta, ev, q, prev, ec, pv, pc, w, b)


def solution(mesh):
    return jax.shard_map(
        per_device,
        mesh=mesh,
        in_specs=(
            P(None, "row", "col"),
            P(None, "row", "col"),
            P(),
            P("row"),
            P("col"),
            P(("row", "col"), None),
            P(("row", "col"), None),
            P("row", "col"),
            P("row", "col"),
        ),
        out_specs=(P(None, "row", "col"), P()),
        check_vma=False,
    )
```

```python
import functools

import jax
import jax.numpy as jnp
from jax import lax
from jax.experimental import pallas as pl
from jax.experimental.pallas import tpu as pltpu
from jax.sharding import PartitionSpec as P

MESH = pl.DeviceIdType.MESH
HIGHEST = lax.Precision.HIGHEST
V, C = 256, 1024
EPS = 1e-06
NN = (((1,), (0,)), ((), ()))
NT = (((1,), (1,)), ((), ()))
TN = (((0,), (0,)), ((), ()))


def halves(a):
    hi = a.astype(jnp.bfloat16)
    return hi, (a - hi.astype(jnp.float32)).astype(jnp.bfloat16)


def left3(a, axis):
    hi, lo = halves(a)
    return jnp.concatenate([hi, lo, hi], axis=axis)


def right3(a, axis):
    hi, lo = halves(a)
    return jnp.concatenate([hi, hi, lo], axis=axis)


def dot(a, b, dims):
    return lax.dot_general(a, b, dims, preferred_element_type=jnp.float32)


def exact(a, b, dims):
    return lax.dot_general(a, b, dims, precision=HIGHEST, preferred_element_type=jnp.float32)


def kernel(
    beta_hbm, ev_hbm, q_hbm, prev_hbm, ec_hbm, pv_hbm, pc_hbm, w_hbm, b_hbm,
    out_ref,
    beta_ref, ev_ref, ec_ref, q_ref, prev_ref, own_pv, pc_other, w_ref, b_ref, pcr, pch, pcl, pv2, xg, pvc, ph, pl_,
    ap, ao, asum, aown, amps, dmine, dc, potx, pot0, ee, eo, dd, kb, r1a, r1b, acc1, r3,
    tz, txy, az, axy, mid, amid, dummy,
    load_sem, send_sem,
    x1r, x2r, x3r, p2r, p3r, p4r, cr, vr, ar_, a3r, dr, q0r, er, f1r, f3r, tr,
):
    row, col = lax.axis_index("row"), lax.axis_index("col")
    x, zhi, y = row // 8, (row // 4) % 2, row % 4
    zlo, core = col // 2, col % 2
    z = zhi * 4 + zlo
    other = 1 - core
    a, b = jnp.where(core == 0, y, x), jnp.where(core == 0, x, y)

    def dev(px, py, pz, pcore):
        return (px * 8 + (pz // 4) * 4 + py, (pz % 4) * 2 + pcore)

    def rc(src, dst, group, rs, to):
        return pltpu.make_async_remote_copy(
            src_ref=src, dst_ref=dst, send_sem=send_sem.at[group], recv_sem=rs, device_id=to, device_id_type=MESH
        )

    def px(d):
        return (x + d) % 4

    def py(d):
        return (y + d) % 4

    def pz(d):
        return (z + d) % 8

    def ab(da, db, dz=0):
        ja, jb = (a + da) % 4, (b + db) % 4
        return dev(jnp.where(core == 0, jb, ja), jnp.where(core == 0, ja, jb), pz(dz), core)

    partner = dev(x, y, z, other)

    def arrived(rs, kib):
        part = dummy.at[pl.ds(0, kib * 2)]
        rc(part, part, 0, rs, partner).wait_recv()

    def left(group, kib):
        part = dummy.at[pl.ds(0, kib * 2)]
        rc(part, part, group, x1r, partner).wait_send()

    def rows_arrived(rs, ref, n):
        part = ref.at[pl.ds(0, n)]
        rc(part, part, 0, rs, partner).wait_recv()

    def rows_left(group, ref, n):
        part = ref.at[pl.ds(0, n)]
        rc(part, part, group, x1r, partner).wait_send()

    lanes = [slice(c * 128, (c + 1) * 128) for c in range(4)]
    pairs = [(q_hbm, q_ref), (pv_hbm, own_pv)]
    for c in range(4):
        mine, its = (pl.ds(pl.multiple_of((c * 2 + k) * 128, 128), 128) for k in (core, other))
        pairs.append((pc_hbm.at[:, mine], pcr.at[zlo, core, :, lanes[c]]))
        pairs.append((pc_hbm.at[:, its], pc_other.at[:, lanes[c]]))
    pairs += [(prev_hbm, prev_ref), (ec_hbm, ec_ref), (ev_hbm, ev_ref), (beta_hbm, beta_ref)]
    pairs += [(w_hbm, w_ref), (b_hbm, b_ref)]
    loads = [pltpu.make_async_copy(s, d, load_sem.at[i]) for i, (s, d) in enumerate(pairs)]
    for c in loads:
        c.start()

    barrier = pltpu.get_barrier_semaphore()

    def greet(to):
        pl.semaphore_signal(barrier, inc=1, device_id=to, device_id_type=MESH)

    in_own_block = (x == zlo) & (core == zhi)
    own_unit = (x == 0) & (zlo == 0) & (core == zhi)
    for c in range(2):
        to = dev(zlo, y, core * 4 + (x - zlo + 4) % 4, (core + c) % 2)
        if c == 0:
            pl.when(jnp.logical_not(own_unit))(functools.partial(greet, to))
        else:
            greet(to)
    for d in range(1, 4):
        greet(dev(px(d), y, z, core))
        greet(dev(x, py(d), z, core))
    for d in (4, 3, 5, 2, 6, 1, 7):
        greet(dev(x, y, pz(d), core))
        greet(dev(x, y, pz(d), other))
    greet(partner)
    loads[0].wait()
    xg[x, zhi, y, zlo] = q_ref[0]
    for i in range(1, 10):
        loads[i].wait()

    @pl.when(own_unit)
    def _():
        pvc[y, zlo, core] = own_pv[...]
        pl.semaphore_wait(barrier, 21 + 1)

    @pl.when(jnp.logical_not(own_unit))
    def _():
        pl.semaphore_wait(barrier, 21 + 2)

    for d in (4, 3, 5, 2, 6, 1, 7):
        rc(q_ref.at[0], xg.at[x, zhi, y, zlo], 0, x1r, dev(x, y, pz(d), core)).start()

    for i in range(2):
        copy = rc(own_pv, pvc.at[y, zlo, core], 2, p2r, dev((x + zlo) % 4, y, x + 4 * ((zhi + i) % 2), zhi))
        if i == 0:
            pl.when(jnp.logical_not(own_unit))(copy.start)
        else:
            copy.start()

    def inside(s):
        return (zlo + s >= 0) & (zlo + s < 4)

    own_rows = pcr.at[zlo, core]
    rc(pc_other, own_rows, 1, cr.at[3, 1], partner).start()
    rc(own_pv, pv2.at[core], 2, vr, partner).start()
    pv2[core] = own_pv[...]
    def rows_came(s, kind):
        part = pcr.at[zlo - s, core if kind == 0 else other]
        rc(part, part, 3, cr.at[s + 3, kind], partner).wait_recv()

    arrived(x1r, 28)

    part = xg.at[x, :, y]
    for d in (2, 1, 3):
        rc(part, part, 0, x2r, ab(d, 0)).start()

    def two(wait, sem, extra=0):
        @pl.when(own_unit)
        def _():
            wait(sem, 64 + extra)

        @pl.when(jnp.logical_not(own_unit))
        def _():
            wait(sem, 128 + extra)

    two(arrived, p2r)

    def place(ja, jb):
        return jnp.where(core == 0, ja, jb), (jnp.where(core == 0, jb, ja) - zlo + 4) % 4

    def unit(da, db):
        return pvc.at[place((a + da) % 4, (b + db) % 4)]

    def p3(d):
        return rc(unit(0, 0), unit(0, 0), 5, p3r.at[d], ab(d, 0))

    def p4(d, rel):
        return rc(unit(rel, 0), unit(rel, 0), 7 if d == 2 else 6, p4r.at[d], ab(0, d))

    for d in (2, 1, 3):
        p3(d).start()
    for d in (1, 3, 2):
        p4(d, 0).start()
    for s in (1, -1):

        @pl.when(inside(s))
        def _():
            rc(own_rows, own_rows, 3, cr.at[s + 3, 0], (row, (zlo + s) * 2 + core)).start()
            rc(pc_other, own_rows, 3, cr.at[s + 3, 1], (row, (zlo + s) * 2 + other)).start()

    arrived(x2r, 96)

    def chunk(c, d):
        return xg.at[px(d)] if c == 0 else xg.at[:, :, py(d)]

    for c in range(2):

        @pl.when(core == c)
        def _():
            for d in (2, 1, 3):
                rc(chunk(c, 0), chunk(c, 0), 8, x3r, ab(0, d)).start()

    for d in (1, 3, 2):
        part = unit(4 - d, 0)
        rc(part, part, 5, p3r.at[d], partner).wait_recv()
        p4(1, 4 - d).start()
        p4(3, 4 - d).start()
    for rel in (3, 1, 2):
        p4(2, rel).start()

    def take_rows(s):
        step = 1 if s > 0 else -1

        @pl.when(inside(-s))
        def _():
            for kind in range(2):
                rows_came(s, kind)

                if abs(s) < 3:

                    @pl.when(inside(step))
                    def _():
                        part = pcr.at[zlo - s, core if kind == 0 else other]
                        rc(part, part, 9, cr.at[s + step + 3, kind], (row, (zlo + step) * 2 + core)).start()

    take_rows(1)
    take_rows(-1)
    arrived(x3r, 384)
    rows_came(0, 1)

    xs = left3(jnp.concatenate([xg[:, :, :, c].reshape(V, 128) for c in range(4)], axis=1), 1)

    def a1(zl):
        return rc(ap.at[zl], ao.at[zl], 10, ar_.at[zl], partner)

    def amp_of(zl):
        at = pl.ds(pl.multiple_of(zl * 128, 128), 128)
        hi, lo = halves(pcr[zl].reshape(128, 512))
        pch[at] = hi
        pcl[at] = lo
        ap[zl] = dot(jnp.concatenate([hi, hi, lo], axis=1), xs, NT).reshape(2, 64, V)
        a1(zl).start()

    amp_of(zlo)

    for s in (1, -1):
        pl.when(inside(-s))(functools.partial(amp_of, zlo - s))

    a1(zlo).wait_recv()
    asum[zlo] = ap[zlo] + ao[zlo]
    own_amp = asum[zlo]
    arrived(vr, 64)
    dens = (pv2[...] * own_amp).reshape(128, V)
    dmine[...] = exact(jnp.ones((8, V), jnp.float32), dens, NT)[0:1]
    at_end = (zlo == 0) | (zlo == 3)

    @pl.when(at_end)
    def _():
        aown[...] = asum[zlo, core]
        for c in (core, other):
            rc(aown, asum.at[zlo, core], 1, a3r, (row, (3 - zlo) * 2 + c)).start()

    slot = y * 4 + zlo
    own_row = in_own_block & (core == 0)

    def density_to(dx, dy, h):
        to = dev(px(dx), py(dy), x + 4 * ((zhi + h) % 2), zhi)
        rc(dmine, dc.at[slot], 11, dr, to).start()

    @pl.when(core == 1)
    def _():
        for i in range(24):
            density_to((2, 1, 3)[i // 8], (i // 2 + 2) % 4, i % 2)

    @pl.when(core == 0)
    def _():
        for i in range(7):
            density_to(0, (2, 2, 1, 1, 3, 3, 0)[i], (0, 1, 0, 1, 0, 1, 1)[i])

        @pl.when(own_row)
        def _():
            dc[slot] = dmine[...]

        pl.when(jnp.logical_not(own_row))(functools.partial(density_to, 0, 0, 0))

    take_rows(2)
    take_rows(-2)
    for s in (2, -2):
        pl.when(inside(-s))(functools.partial(amp_of, zlo - s))

    near = zlo // 2
    far = 1 - near

    def use(zl):
        amps[pl.ds(pl.multiple_of(zl * 128, 128), 128)] = left3(asum[zl].reshape(128, V), 1)

    def join(zl):
        a1(zl).wait_recv()
        asum[zl] = ap[zl] + ao[zl]
        use(zl)

    use(zlo)
    join(near * 2 + 1 - zlo % 2)

    loads[14].wait()

    def split(d):
        hi, lo = halves(jnp.concatenate([pvc[place(j, (b + d) % 4)].reshape(128, V) for j in range(4)], axis=0))
        ph[d] = hi
        pl_[d] = lo

    def block(d, pair):
        hi, lo = ph[d], pl_[d]
        rows = pl.ds(pl.multiple_of(pair * 256, 256), 256)
        spots = [place(j, (b + d) % 4) for j in range(4)]
        columns = [pl.ds(pl.multiple_of(ys * 512 + zs * 128, 128), 128) for ys, zs in spots]
        weights = jnp.concatenate([w_ref[rows, at] for at in columns], axis=1)
        terms = dot(amps[rows], jnp.concatenate([hi, hi, lo], axis=1), NT) * weights
        return dot(left3(terms, 1), jnp.concatenate([hi, hi, lo], axis=0), NN)

    def e1(i, pair):
        part = pl.ds(2 * pair, 2)
        return rc(ee.at[part], eo.at[part], 13, er.at[i], partner)

    split(0)
    part = block(0, near)
    arrived(p4r.at[1], 512)
    split(3)
    part = part + block(3, near)
    arrived(p4r.at[3], 512)
    split(1)
    part = part + block(1, near)
    ee[pl.ds(2 * near, 2)] = part.reshape(2, 2, 64, V)
    arrived(p4r.at[2], 512)
    split(2)
    ee[pl.ds(2 * near, 2)] += block(2, near).reshape(2, 2, 64, V)
    e1(0, near).start()

    loads[15].wait()

    @pl.when(own_row)
    def _():
        rows_arrived(dr, dc, 15)

    @pl.when(jnp.logical_not(own_row))
    def _():
        rows_arrived(dr, dc, 16)

    pot = None
    for t in range(16):
        piece = b_ref[:, t * 128 : (t + 1) * 128] * dc[t]
        pot = piece if pot is None else pot + piece
    pot = jnp.sum(pot, axis=1, keepdims=True)
    diag = lax.broadcasted_iota(jnp.int32, (128, 128), 0) == lax.broadcasted_iota(jnp.int32, (128, 128), 1)
    for j in range(4):
        potx[j] = jnp.sum(jnp.where(diag, pot[j * 128 : (j + 1) * 128], 0.0), axis=0, keepdims=True)
    for d in (2, 1, 3, 0):
        zl = (zlo + d) % 4
        for c in range(2):
            if d or c:
                rc(potx.at[zl], pot0.at[2 * d + c], 15, q0r, (row, zl * 2 + (core + c) % 2)).start()
    pot0[0] = potx[zlo]
    for s in (2, -2):
        pl.when(inside(-s))(functools.partial(join, zlo - s))

    @pl.when(at_end)
    def _():
        arrived(a3r, 128)
        use(3 - zlo)

    @pl.when(jnp.logical_not(at_end))
    def _():
        join(3 - zlo)

    part = block(0, far) + block(3, far) + block(1, far) + block(2, far)
    ee[pl.ds(2 * far, 2)] = part.reshape(2, 2, 64, V)
    e1(1, far).start()

    for s in (3, -3):
        take_rows(s)

        @pl.when(inside(-s))
        def _():
            at = pl.ds(pl.multiple_of((zlo - s) * 128, 128), 128)
            hi, lo = halves(pcr[zlo - s].reshape(128, 512))
            pch[at] = hi
            pcl[at] = lo

    def kpart(i, pair):
        e1(i, pair).wait_recv()
        at = pl.ds(2 * pair, 2)
        both = -(ee[at] + eo[at])
        dd[at] = both
        rows = pl.ds(pl.multiple_of(pair * 256, 256), 256)
        hi, lo = pch[rows], pcl[rows]
        return dot(left3(both.reshape(256, V), 0), jnp.concatenate([hi, hi, lo], axis=0), TN)

    kfull = kpart(0, near)
    kfull = kfull + kpart(1, far)
    rows_arrived(q0r, pot0, 7)
    pot_row = jnp.sum(pot0[...], axis=0)
    pot2 = 2.0 * jnp.sum(jnp.where(diag, pot_row, 0.0), axis=1, keepdims=True)
    bare = pot2 * pv2[...].reshape(128, V)
    rows = pl.ds(pl.multiple_of(zlo * 128, 128), 128)
    hi, lo = pch[rows], pcl[rows]
    kfull = kfull + dot(left3(bare, 0), jnp.concatenate([hi, hi, lo], axis=0), TN)
    dd[zlo] = dd[zlo] + bare.reshape(2, 64, V)
    for c in range(4):
        kb[:, :, :, c] = kfull[:, lanes[c]].reshape(4, 2, 4, 8, 128)

    for c in range(2):

        @pl.when(core == c)
        def _():
            for d in (2, 1, 3):
                part = kb.at[px(d)] if c == 0 else kb.at[:, :, py(d)]
                rc(part, (r1a if c == 0 else r1b).at[d - 1], 16, f1r, ab(0, d)).start()

    for i in (10, 11, 12, 13):
        loads[i].wait()
    q, prev = q_ref[0], prev_ref[0]
    sub8 = lax.broadcasted_iota(jnp.int32, (8, 128), 0)
    ev = jnp.zeros((8, 128), jnp.float32)
    for i in range(8):
        ev = jnp.where(sub8 == i, ev_ref[i], ev)
    gaps = ec_ref[...].reshape(1, 128) - ev
    prod = (dd[:, core] * asum[:, core]).reshape(256, V)
    prod = jnp.sum(prod[:, 0:128] + prod[:, 128:256], axis=0, keepdims=True)
    qq = jnp.sum(q * q, axis=0, keepdims=True)
    qu = prod + jnp.sum(gaps * q * q, axis=0, keepdims=True)
    az[0] = jnp.concatenate([qu, qq], axis=1)

    def t1(src, dst, group, rs):
        for d in (4, 3, 5, 2, 6, 1, 7, 0):
            for j in (d, d + 8):
                if j:
                    to = dev(x, y, pz(d), core if j < 8 else other)
                    rc(src, dst.at[j], group, rs, to).start()

    def t2(src, dst, group, rs):
        for j in (10, 9, 11, 6, 14, 2, 8, 5, 7, 13, 15, 1, 3, 4, 12):
            rc(src, dst.at[j], group, rs, dev(px(j // 4), py(j % 4), z, core)).start()

    t1(az.at[0], az, 18, tr.at[0])

    arrived(f1r, 384)
    for c in range(2):

        @pl.when(core == c)
        def _():
            if c == 0:
                for i in range(2):
                    acc1[:, i] = kb[x, i] + r1a[0, i] + r1a[1, i] + r1a[2, i]
            else:
                acc1[...] = kb[:, :, y] + r1b[0] + r1b[1] + r1b[2]

    for da in (2, 1, 3, 0):
        for dz in (4, 3, 5, 2, 6, 1, 7, 0):
            if da or dz:
                zz = pz(dz)
                part = acc1.at[(a + da) % 4, zz // 4, zz % 4]
                rc(part, r3.at[da * 8 + dz], 17, f3r, ab(da, 0, dz)).start()
    rows_arrived(tr.at[0], az, 15)
    amid[...] = jnp.sum(az[...], axis=0)
    axy[0] = amid[...]
    t2(amid, axy, 19, tr.at[1])
    arrived(f3r, 124)
    tile = acc1[a, zhi, zlo] + jnp.sum(r3[1:32], axis=0)
    inv = 1.0 / (V * C)
    bp = beta_ref[...]
    rows_arrived(tr.at[1], axy, 15)
    total = jnp.sum(axy[...], axis=0)
    qu = jnp.sum(total[:, 0:128], axis=1, keepdims=True)
    qq = jnp.sum(total[:, 128:256], axis=1, keepdims=True)
    alpha = qu * inv / (qq * inv + EPS)
    resid = tile + (gaps - alpha) * q - bp * prev
    tz[0] = jnp.sum(resid * resid, axis=0, keepdims=True)
    t1(tz.at[0], tz, 20, tr.at[2])
    rows_arrived(tr.at[2], tz, 15)
    mid[...] = jnp.sum(tz[...], axis=0)
    t2(mid, txy, 21, tr.at[3])
    txy[0] = mid[...]
    rows_arrived(tr.at[3], txy, 15)
    ww = jnp.sum(jnp.sum(txy[...], axis=0), axis=1, keepdims=True)
    beta = jnp.sqrt(ww * inv + EPS)
    out_ref[0:8] = resid / beta
    out_ref[8:16] = jnp.where(lax.broadcasted_iota(jnp.int32, (8, 128), 1) == 0, alpha, beta)

    left(0, 124)
    two(left, 2, 64)
    left(5, 384)
    left(6, 1024)
    left(7, 512)
    left(8, 384)

    @pl.when((zlo == 0) | (zlo == 3))
    def _():
        left(1, 256)
        left(3, 256)
        left(10, 384)

    @pl.when((zlo == 1) | (zlo == 2))
    def _():
        left(1, 128)
        left(3, 512)
        left(9, 768)
        left(10, 512)


    @pl.when(core == 1)
    def _():
        left(11, 12)

    @pl.when(core == 0)
    def _():
        pl.when(own_row)(lambda: rows_left(11, dc, 7))
        pl.when(jnp.logical_not(own_row))(lambda: rows_left(11, dc, 8))

    left(13, 512)
    rows_left(15, pot0, 7)
    left(16, 384)
    left(17, 124)
    rows_left(18, az, 15)
    rows_left(19, axy, 15)
    rows_left(20, tz, 15)
    rows_left(21, txy, 15)


def split_results(both_ref, out_ref, coef_ref):
    out_ref[0] = both_ref[0:8]
    coef_ref[...] = both_ref[8:9, 0:2]


def per_device(q, prev, beta, ev, ec, pv, pc, w, b):
    f32 = jnp.float32
    vmem = pl.BlockSpec(memory_space=pltpu.VMEM)
    hbm = pl.BlockSpec(memory_space=pltpu.HBM)

    def buf(*shape):
        return pltpu.VMEM(shape, f32)

    def sem(*n):
        return pltpu.SemaphoreType.DMA(n)

    tile = (8, 128)
    bf16 = jnp.bfloat16
    scratch = [
        buf(1, 1), pltpu.SMEM((8,), f32), buf(128),
        buf(1, *tile), buf(1, *tile), buf(64, V), buf(64, 512), buf(512, 2048), buf(512, 2048),
        buf(4, 2, 64, 512), pltpu.VMEM((512, 512), bf16), pltpu.VMEM((512, 512), bf16), buf(2, 64, V),
        buf(4, 2, 4, 4, *tile), buf(4, 4, 2, 64, V), pltpu.VMEM((4, 512, V), bf16), pltpu.VMEM((4, 512, V), bf16),
        buf(4, 2, 64, V), buf(4, 2, 64, V), buf(4, 2, 64, V), buf(64, V), pltpu.VMEM((512, 3 * V), bf16),
        buf(1, 128), buf(16, 1, 128), buf(4, 1, 128), buf(8, 1, 128),
        buf(4, 2, 64, V), buf(4, 2, 64, V), buf(4, 2, 64, V),
        buf(4, 2, 4, 4, *tile), buf(3, 2, 4, 4, *tile), buf(3, 4, 2, 4, *tile), buf(4, 2, 4, *tile), buf(32, *tile),
        buf(16, 1, 128), buf(16, 1, 128), buf(16, 1, 256), buf(16, 1, 256), buf(1, 128), buf(1, 256), buf(2048, 128),
        sem(16), sem(22),
        sem(), sem(), sem(), sem(), sem(4), sem(4), sem(7, 2), sem(), sem(4), sem(), sem(), sem(),
        sem(2), sem(), sem(), sem(4),
    ]
    both = pl.pallas_call(
        kernel,
        out_shape=jax.ShapeDtypeStruct((16, 128), f32),
        in_specs=[hbm] * 9,
        out_specs=vmem,
        scratch_shapes=scratch,
        compiler_params=pltpu.CompilerParams(
            collective_id=0, has_side_effects=True, vmem_limit_bytes=60 * 1024 * 1024
        ),
        name="lanczos_step",
    )(beta.reshape(1, 1), ev, q, prev, ec, pv, pc, w, b)
    return pl.pallas_call(
        split_results,
        out_shape=(jax.ShapeDtypeStruct((1, 8, 128), f32), jax.ShapeDtypeStruct((1, 2), f32)),
        in_specs=[vmem],
        out_specs=(vmem, vmem),
        name="split_results",
    )(both)


def solution(mesh):
    return jax.shard_map(
        per_device,
        mesh=mesh,
        in_specs=(
            P(None, "row", "col"),
            P(None, "row", "col"),
            P(),
            P("row"),
            P("col"),
            P(("row", "col"), None),
            P(("row", "col"), None),
            P("row", "col"),
            P("row", "col"),
        ),
        out_specs=(P(None, "row", "col"), P()),
        check_vma=False,
    )
```

```python
import functools

import jax
import jax.numpy as jnp
from jax import lax
from jax.experimental import pallas as pl
from jax.experimental.pallas import tpu as pltpu
from jax.sharding import PartitionSpec as P

MESH = pl.DeviceIdType.MESH
HIGHEST = lax.Precision.HIGHEST
V, C = 256, 1024
EPS = 1e-06
NN = (((1,), (0,)), ((), ()))
NT = (((1,), (1,)), ((), ()))
TN = (((0,), (0,)), ((), ()))


def halves(a):
    hi = a.astype(jnp.bfloat16)
    return hi, (a - hi.astype(jnp.float32)).astype(jnp.bfloat16)


def left3(a, axis):
    hi, lo = halves(a)
    return jnp.concatenate([hi, lo, hi], axis=axis)


def right3(a, axis):
    hi, lo = halves(a)
    return jnp.concatenate([hi, hi, lo], axis=axis)


def dot(a, b, dims):
    return lax.dot_general(a, b, dims, preferred_element_type=jnp.float32)


def exact(a, b, dims):
    return lax.dot_general(a, b, dims, precision=HIGHEST, preferred_element_type=jnp.float32)


def kernel(
    beta_hbm, ev_hbm, q_hbm, prev_hbm, ec_hbm, pv_hbm, pc_hbm, w_hbm, b_hbm,
    out_ref,
    beta_ref, ev_ref, ec_ref, q_ref, prev_ref, own_pv, pc_other, w_ref, b_ref, pcr, pch, pcl, pv2, xg, pvc, ph, pl_,
    ap, ao, asum, aown, amps, dmine, dc, potx, pot0, ee, eo, dd, kb, r1a, r1b, acc1, r3,
    tz, txy, az, axy, mid, amid, dummy,
    load_sem, send_sem,
    x1r, x2r, x3r, p2r, p3r, p4r, cr, vr, ar_, a3r, dr, q0r, er, f1r, f3r, tr,
):
    row, col = lax.axis_index("row"), lax.axis_index("col")
    x, zhi, y = row // 8, (row // 4) % 2, row % 4
    zlo, core = col // 2, col % 2
    z = zhi * 4 + zlo
    other = 1 - core
    a, b = jnp.where(core == 0, y, x), jnp.where(core == 0, x, y)

    def dev(px, py, pz, pcore):
        return (px * 8 + (pz // 4) * 4 + py, (pz % 4) * 2 + pcore)

    def rc(src, dst, group, rs, to):
        return pltpu.make_async_remote_copy(
            src_ref=src, dst_ref=dst, send_sem=send_sem.at[group], recv_sem=rs, device_id=to, device_id_type=MESH
        )

    def px(d):
        return (x + d) % 4

    def py(d):
        return (y + d) % 4

    def pz(d):
        return (z + d) % 8

    def ab(da, db, dz=0):
        ja, jb = (a + da) % 4, (b + db) % 4
        return dev(jnp.where(core == 0, jb, ja), jnp.where(core == 0, ja, jb), pz(dz), core)

    partner = dev(x, y, z, other)

    def arrived(rs, kib):
        part = dummy.at[pl.ds(0, kib * 2)]
        rc(part, part, 0, rs, partner).wait_recv()

    def left(group, kib):
        part = dummy.at[pl.ds(0, kib * 2)]
        rc(part, part, group, x1r, partner).wait_send()

    def rows_arrived(rs, ref, n):
        part = ref.at[pl.ds(0, n)]
        rc(part, part, 0, rs, partner).wait_recv()

    def rows_left(group, ref, n):
        part = ref.at[pl.ds(0, n)]
        rc(part, part, group, x1r, partner).wait_send()

    lanes = [slice(c * 128, (c + 1) * 128) for c in range(4)]
    pairs = [(q_hbm, q_ref), (pv_hbm, own_pv)]
    for c in range(4):
        mine, its = (pl.ds(pl.multiple_of((c * 2 + k) * 128, 128), 128) for k in (core, other))
        pairs.append((pc_hbm.at[:, mine], pcr.at[zlo, core, :, lanes[c]]))
        pairs.append((pc_hbm.at[:, its], pc_other.at[:, lanes[c]]))
    pairs += [(prev_hbm, prev_ref), (ec_hbm, ec_ref), (ev_hbm, ev_ref), (beta_hbm, beta_ref)]
    pairs += [(w_hbm, w_ref), (b_hbm, b_ref)]
    loads = [pltpu.make_async_copy(s, d, load_sem.at[i]) for i, (s, d) in enumerate(pairs)]
    for c in loads:
        c.start()

    barrier = pltpu.get_barrier_semaphore()

    def greet(to):
        pl.semaphore_signal(barrier, inc=1, device_id=to, device_id_type=MESH)

    in_own_block = (x == zlo) & (core == zhi)
    own_unit = (x == 0) & (zlo == 0) & (core == zhi)
    for c in range(2):
        to = dev(zlo, y, core * 4 + (x - zlo + 4) % 4, (core + c) % 2)
        if c == 0:
            pl.when(jnp.logical_not(own_unit))(functools.partial(greet, to))
        else:
            greet(to)
    for d in range(1, 4):
        greet(dev(px(d), y, z, core))
        greet(dev(x, py(d), z, core))
    for d in (4, 3, 5, 2, 6, 1, 7):
        greet(dev(x, y, pz(d), core))
        greet(dev(x, y, pz(d), other))
    greet(partner)
    loads[0].wait()
    xg[x, zhi, y, zlo] = q_ref[0]
    for i in range(1, 10):
        loads[i].wait()

    @pl.when(own_unit)
    def _():
        pvc[y, zlo, core] = own_pv[...]
        pl.semaphore_wait(barrier, 21 + 1)

    @pl.when(jnp.logical_not(own_unit))
    def _():
        pl.semaphore_wait(barrier, 21 + 2)

    for d in (4, 3, 5, 2, 6, 1, 7):
        rc(q_ref.at[0], xg.at[x, zhi, y, zlo], 0, x1r, dev(x, y, pz(d), core)).start()

    for i in range(2):
        copy = rc(own_pv, pvc.at[y, zlo, core], 2, p2r, dev((x + zlo) % 4, y, x + 4 * ((zhi + i) % 2), zhi))
        if i == 0:
            pl.when(jnp.logical_not(own_unit))(copy.start)
        else:
            copy.start()

    def inside(s):
        return (zlo + s >= 0) & (zlo + s < 4)

    own_rows = pcr.at[zlo, core]
    rc(pc_other, own_rows, 1, cr.at[3, 1], partner).start()
    rc(own_pv, pv2.at[core], 2, vr, partner).start()
    pv2[core] = own_pv[...]
    def rows_came(s, kind):
        part = pcr.at[zlo - s, core if kind == 0 else other]
        rc(part, part, 3, cr.at[s + 3, kind], partner).wait_recv()

    arrived(x1r, 28)

    part = xg.at[x, :, y]
    for d in (2, 1, 3):
        rc(part, part, 0, x2r, ab(d, 0)).start()

    def two(wait, sem, extra=0):
        @pl.when(own_unit)
        def _():
            wait(sem, 64 + extra)

        @pl.when(jnp.logical_not(own_unit))
        def _():
            wait(sem, 128 + extra)

    two(arrived, p2r)

    def place(ja, jb):
        return jnp.where(core == 0, ja, jb), (jnp.where(core == 0, jb, ja) - zlo + 4) % 4

    def unit(da, db):
        return pvc.at[place((a + da) % 4, (b + db) % 4)]

    def p3(d):
        return rc(unit(0, 0), unit(0, 0), 5, p3r.at[d], ab(d, 0))

    def p4(d, rel):
        return rc(unit(rel, 0), unit(rel, 0), 7 if d == 2 else 6, p4r.at[d], ab(0, d))

    for d in (2, 1, 3):
        p3(d).start()
    for s in (1, -1):

        @pl.when(inside(s))
        def _():
            rc(own_rows, own_rows, 3, cr.at[s + 3, 0], (row, (zlo + s) * 2 + core)).start()
            rc(pc_other, own_rows, 3, cr.at[s + 3, 1], (row, (zlo + s) * 2 + other)).start()

    arrived(x2r, 96)

    def chunk(c, d):
        return xg.at[px(d)] if c == 0 else xg.at[:, :, py(d)]

    for c in range(2):

        @pl.when(core == c)
        def _():
            for d in (2, 1, 3):
                rc(chunk(c, 0), chunk(c, 0), 8, x3r, ab(0, d)).start()

    def take_rows(s):
        step = 1 if s > 0 else -1

        @pl.when(inside(-s))
        def _():
            for kind in range(2):
                rows_came(s, kind)

                if abs(s) < 3:

                    @pl.when(inside(step))
                    def _():
                        part = pcr.at[zlo - s, core if kind == 0 else other]
                        rc(part, part, 9, cr.at[s + step + 3, kind], (row, (zlo + step) * 2 + core)).start()

    def pass_units():
        for d in (1, 3, 2):
            part = unit(4 - d, 0)
            rc(part, part, 5, p3r.at[d], partner).wait_recv()
            p4(1, 4 - d).start()
            p4(3, 4 - d).start()
        for rel in (3, 1, 2):
            p4(2, rel).start()

    for d in (1, 3, 2):
        p4(d, 0).start()

    pl.when(core == 1)(pass_units)
    take_rows(1)
    take_rows(-1)
    pl.when(core == 0)(pass_units)
    arrived(x3r, 384)
    rows_came(0, 1)

    xs = left3(jnp.concatenate([xg[:, :, :, c].reshape(V, 128) for c in range(4)], axis=1), 1)

    def a1(zl):
        return rc(ap.at[zl], ao.at[zl], 10, ar_.at[zl], partner)

    def amp_of(zl):
        at = pl.ds(pl.multiple_of(zl * 128, 128), 128)
        hi, lo = halves(pcr[zl].reshape(128, 512))
        pch[at] = hi
        pcl[at] = lo
        ap[zl] = dot(jnp.concatenate([hi, hi, lo], axis=1), xs, NT).reshape(2, 64, V)
        a1(zl).start()

    amp_of(zlo)

    for s in (1, -1):
        pl.when(inside(-s))(functools.partial(amp_of, zlo - s))

    a1(zlo).wait_recv()
    asum[zlo] = ap[zlo] + ao[zlo]
    own_amp = asum[zlo]
    arrived(vr, 64)
    dens = (pv2[...] * own_amp).reshape(128, V)
    dmine[...] = exact(jnp.ones((8, V), jnp.float32), dens, NT)[0:1]
    at_end = (zlo == 0) | (zlo == 3)

    @pl.when(at_end)
    def _():
        aown[...] = asum[zlo, core]
        for c in (core, other):
            rc(aown, asum.at[zlo, core], 1, a3r, (row, (3 - zlo) * 2 + c)).start()

    slot = y * 4 + zlo
    own_row = in_own_block & (core == 0)

    def density_to(dx, dy, h):
        to = dev(px(dx), py(dy), x + 4 * ((zhi + h) % 2), zhi)
        rc(dmine, dc.at[slot], 11, dr, to).start()

    @pl.when(core == 1)
    def _():
        for i in range(24):
            density_to((2, 1, 3)[i // 8], (i // 2 + 2) % 4, i % 2)

    @pl.when(core == 0)
    def _():
        for i in range(7):
            density_to(0, (2, 2, 1, 1, 3, 3, 0)[i], (0, 1, 0, 1, 0, 1, 1)[i])

        @pl.when(own_row)
        def _():
            dc[slot] = dmine[...]

        pl.when(jnp.logical_not(own_row))(functools.partial(density_to, 0, 0, 0))

    near = zlo // 2
    far = 1 - near

    def use(zl):
        amps[pl.ds(pl.multiple_of(zl * 128, 128), 128)] = left3(asum[zl].reshape(128, V), 1)

    def join(zl):
        a1(zl).wait_recv()
        asum[zl] = ap[zl] + ao[zl]
        use(zl)

    use(zlo)
    join(near * 2 + 1 - zlo % 2)

    loads[14].wait()

    def split(d):
        hi, lo = halves(jnp.concatenate([pvc[place(j, (b + d) % 4)].reshape(128, V) for j in range(4)], axis=0))
        ph[d] = hi
        pl_[d] = lo

    def block(d, pair):
        hi, lo = ph[d], pl_[d]
        rows = pl.ds(pl.multiple_of(pair * 256, 256), 256)
        spots = [place(j, (b + d) % 4) for j in range(4)]
        columns = [pl.ds(pl.multiple_of(ys * 512 + zs * 128, 128), 128) for ys, zs in spots]
        weights = jnp.concatenate([w_ref[rows, at] for at in columns], axis=1)
        terms = dot(amps[rows], jnp.concatenate([hi, hi, lo], axis=1), NT) * weights
        return dot(left3(terms, 1), jnp.concatenate([hi, hi, lo], axis=0), NN)

    def e1(i, pair):
        part = pl.ds(2 * pair, 2)
        return rc(ee.at[part], eo.at[part], 13, er.at[i], partner)

    split(0)
    part = block(0, near)
    take_rows(2)
    take_rows(-2)
    for s in (2, -2):
        pl.when(inside(-s))(functools.partial(amp_of, zlo - s))

    arrived(p4r.at[1], 512)
    split(3)
    part = part + block(3, near)
    arrived(p4r.at[3], 512)
    split(1)
    part = part + block(1, near)
    ee[pl.ds(2 * near, 2)] = part.reshape(2, 2, 64, V)
    arrived(p4r.at[2], 512)
    split(2)
    ee[pl.ds(2 * near, 2)] += block(2, near).reshape(2, 2, 64, V)
    e1(0, near).start()

    loads[15].wait()

    @pl.when(own_row)
    def _():
        rows_arrived(dr, dc, 15)

    @pl.when(jnp.logical_not(own_row))
    def _():
        rows_arrived(dr, dc, 16)

    pot = None
    for t in range(16):
        piece = b_ref[:, t * 128 : (t + 1) * 128] * dc[t]
        pot = piece if pot is None else pot + piece
    pot = jnp.sum(pot, axis=1, keepdims=True)
    diag = lax.broadcasted_iota(jnp.int32, (128, 128), 0) == lax.broadcasted_iota(jnp.int32, (128, 128), 1)
    for j in range(4):
        potx[j] = jnp.sum(jnp.where(diag, pot[j * 128 : (j + 1) * 128], 0.0), axis=0, keepdims=True)
    for d in (2, 1, 3, 0):
        zl = (zlo + d) % 4
        for c in range(2):
            if d or c:
                rc(potx.at[zl], pot0.at[2 * d + c], 15, q0r, (row, zl * 2 + (core + c) % 2)).start()
    pot0[0] = potx[zlo]
    for s in (2, -2):
        pl.when(inside(-s))(functools.partial(join, zlo - s))

    @pl.when(at_end)
    def _():
        arrived(a3r, 128)
        use(3 - zlo)

    @pl.when(jnp.logical_not(at_end))
    def _():
        join(3 - zlo)

    part = block(0, far) + block(3, far) + block(1, far) + block(2, far)
    ee[pl.ds(2 * far, 2)] = part.reshape(2, 2, 64, V)
    e1(1, far).start()

    for s in (3, -3):
        take_rows(s)

        @pl.when(inside(-s))
        def _():
            at = pl.ds(pl.multiple_of((zlo - s) * 128, 128), 128)
            hi, lo = halves(pcr[zlo - s].reshape(128, 512))
            pch[at] = hi
            pcl[at] = lo

    def kpart(i, pair):
        e1(i, pair).wait_recv()
        at = pl.ds(2 * pair, 2)
        both = -(ee[at] + eo[at])
        dd[at] = both
        rows = pl.ds(pl.multiple_of(pair * 256, 256), 256)
        hi, lo = pch[rows], pcl[rows]
        return dot(left3(both.reshape(256, V), 0), jnp.concatenate([hi, hi, lo], axis=0), TN)

    kfull = kpart(0, near)
    kfull = kfull + kpart(1, far)
    rows_arrived(q0r, pot0, 7)
    pot_row = jnp.sum(pot0[...], axis=0)
    pot2 = 2.0 * jnp.sum(jnp.where(diag, pot_row, 0.0), axis=1, keepdims=True)
    bare = pot2 * pv2[...].reshape(128, V)
    rows = pl.ds(pl.multiple_of(zlo * 128, 128), 128)
    hi, lo = pch[rows], pcl[rows]
    kfull = kfull + dot(left3(bare, 0), jnp.concatenate([hi, hi, lo], axis=0), TN)
    dd[zlo] = dd[zlo] + bare.reshape(2, 64, V)
    for c in range(4):
        kb[:, :, :, c] = kfull[:, lanes[c]].reshape(4, 2, 4, 8, 128)

    for c in range(2):

        @pl.when(core == c)
        def _():
            for d in (2, 1, 3):
                part = kb.at[px(d)] if c == 0 else kb.at[:, :, py(d)]
                rc(part, (r1a if c == 0 else r1b).at[d - 1], 16, f1r, ab(0, d)).start()

    for i in (10, 11, 12, 13):
        loads[i].wait()
    q, prev = q_ref[0], prev_ref[0]
    sub8 = lax.broadcasted_iota(jnp.int32, (8, 128), 0)
    ev = jnp.zeros((8, 128), jnp.float32)
    for i in range(8):
        ev = jnp.where(sub8 == i, ev_ref[i], ev)
    gaps = ec_ref[...].reshape(1, 128) - ev
    prod = (dd[:, core] * asum[:, core]).reshape(256, V)
    prod = jnp.sum(prod[:, 0:128] + prod[:, 128:256], axis=0, keepdims=True)
    qq = jnp.sum(q * q, axis=0, keepdims=True)
    qu = prod + jnp.sum(gaps * q * q, axis=0, keepdims=True)
    az[0] = jnp.concatenate([qu, qq], axis=1)

    def t1(src, dst, group, rs):
        for d in (4, 3, 5, 2, 6, 1, 7, 0):
            for j in (d, d + 8):
                if j:
                    to = dev(x, y, pz(d), core if j < 8 else other)
                    rc(src, dst.at[j], group, rs, to).start()

    def t2(src, dst, group, rs):
        for j in (10, 9, 11, 6, 14, 2, 8, 5, 7, 13, 15, 1, 3, 4, 12):
            rc(src, dst.at[j], group, rs, dev(px(j // 4), py(j % 4), z, core)).start()

    t1(az.at[0], az, 18, tr.at[0])

    arrived(f1r, 384)
    for c in range(2):

        @pl.when(core == c)
        def _():
            if c == 0:
                for i in range(2):
                    acc1[:, i] = kb[x, i] + r1a[0, i] + r1a[1, i] + r1a[2, i]
            else:
                acc1[...] = kb[:, :, y] + r1b[0] + r1b[1] + r1b[2]

    for da in (2, 1, 3, 0):
        for dz in (4, 3, 5, 2, 6, 1, 7, 0):
            if da or dz:
                zz = pz(dz)
                part = acc1.at[(a + da) % 4, zz // 4, zz % 4]
                rc(part, r3.at[da * 8 + dz], 17, f3r, ab(da, 0, dz)).start()
    rows_arrived(tr.at[0], az, 15)
    amid[...] = jnp.sum(az[...], axis=0)
    axy[0] = amid[...]
    t2(amid, axy, 19, tr.at[1])
    arrived(f3r, 124)
    tile = acc1[a, zhi, zlo] + jnp.sum(r3[1:32], axis=0)
    inv = 1.0 / (V * C)
    bp = beta_ref[...]
    rows_arrived(tr.at[1], axy, 15)
    total = jnp.sum(axy[...], axis=0)
    qu = jnp.sum(total[:, 0:128], axis=1, keepdims=True)
    qq = jnp.sum(total[:, 128:256], axis=1, keepdims=True)
    alpha = qu * inv / (qq * inv + EPS)
    resid = tile + (gaps - alpha) * q - bp * prev
    tz[0] = jnp.sum(resid * resid, axis=0, keepdims=True)
    t1(tz.at[0], tz, 20, tr.at[2])
    rows_arrived(tr.at[2], tz, 15)
    mid[...] = jnp.sum(tz[...], axis=0)
    t2(mid, txy, 21, tr.at[3])
    txy[0] = mid[...]
    rows_arrived(tr.at[3], txy, 15)
    ww = jnp.sum(jnp.sum(txy[...], axis=0), axis=1, keepdims=True)
    beta = jnp.sqrt(ww * inv + EPS)
    out_ref[0:8] = resid / beta
    out_ref[8:16] = jnp.where(lax.broadcasted_iota(jnp.int32, (8, 128), 1) == 0, alpha, beta)

    left(0, 124)
    two(left, 2, 64)
    left(5, 384)
    left(6, 1024)
    left(7, 512)
    left(8, 384)

    @pl.when((zlo == 0) | (zlo == 3))
    def _():
        left(1, 256)
        left(3, 256)
        left(10, 384)

    @pl.when((zlo == 1) | (zlo == 2))
    def _():
        left(1, 128)
        left(3, 512)
        left(9, 768)
        left(10, 512)


    @pl.when(core == 1)
    def _():
        left(11, 12)

    @pl.when(core == 0)
    def _():
        pl.when(own_row)(lambda: rows_left(11, dc, 7))
        pl.when(jnp.logical_not(own_row))(lambda: rows_left(11, dc, 8))

    left(13, 512)
    rows_left(15, pot0, 7)
    left(16, 384)
    left(17, 124)
    rows_left(18, az, 15)
    rows_left(19, axy, 15)
    rows_left(20, tz, 15)
    rows_left(21, txy, 15)


def split_results(both_ref, out_ref, coef_ref):
    out_ref[0] = both_ref[0:8]
    coef_ref[...] = both_ref[8:9, 0:2]


def per_device(q, prev, beta, ev, ec, pv, pc, w, b):
    f32 = jnp.float32
    vmem = pl.BlockSpec(memory_space=pltpu.VMEM)
    hbm = pl.BlockSpec(memory_space=pltpu.HBM)

    def buf(*shape):
        return pltpu.VMEM(shape, f32)

    def sem(*n):
        return pltpu.SemaphoreType.DMA(n)

    tile = (8, 128)
    bf16 = jnp.bfloat16
    scratch = [
        buf(1, 1), pltpu.SMEM((8,), f32), buf(128),
        buf(1, *tile), buf(1, *tile), buf(64, V), buf(64, 512), buf(512, 2048), buf(512, 2048),
        buf(4, 2, 64, 512), pltpu.VMEM((512, 512), bf16), pltpu.VMEM((512, 512), bf16), buf(2, 64, V),
        buf(4, 2, 4, 4, *tile), buf(4, 4, 2, 64, V), pltpu.VMEM((4, 512, V), bf16), pltpu.VMEM((4, 512, V), bf16),
        buf(4, 2, 64, V), buf(4, 2, 64, V), buf(4, 2, 64, V), buf(64, V), pltpu.VMEM((512, 3 * V), bf16),
        buf(1, 128), buf(16, 1, 128), buf(4, 1, 128), buf(8, 1, 128),
        buf(4, 2, 64, V), buf(4, 2, 64, V), buf(4, 2, 64, V),
        buf(4, 2, 4, 4, *tile), buf(3, 2, 4, 4, *tile), buf(3, 4, 2, 4, *tile), buf(4, 2, 4, *tile), buf(32, *tile),
        buf(16, 1, 128), buf(16, 1, 128), buf(16, 1, 256), buf(16, 1, 256), buf(1, 128), buf(1, 256), buf(2048, 128),
        sem(16), sem(22),
        sem(), sem(), sem(), sem(), sem(4), sem(4), sem(7, 2), sem(), sem(4), sem(), sem(), sem(),
        sem(2), sem(), sem(), sem(4),
    ]
    both = pl.pallas_call(
        kernel,
        out_shape=jax.ShapeDtypeStruct((16, 128), f32),
        in_specs=[hbm] * 9,
        out_specs=vmem,
        scratch_shapes=scratch,
        compiler_params=pltpu.CompilerParams(
            collective_id=0, has_side_effects=True, vmem_limit_bytes=60 * 1024 * 1024
        ),
        name="lanczos_step",
    )(beta.reshape(1, 1), ev, q, prev, ec, pv, pc, w, b)
    return pl.pallas_call(
        split_results,
        out_shape=(jax.ShapeDtypeStruct((1, 8, 128), f32), jax.ShapeDtypeStruct((1, 2), f32)),
        in_specs=[vmem],
        out_specs=(vmem, vmem),
        name="split_results",
    )(both)


def solution(mesh):
    return jax.shard_map(
        per_device,
        mesh=mesh,
        in_specs=(
            P(None, "row", "col"),
            P(None, "row", "col"),
            P(),
            P("row"),
            P("col"),
            P(("row", "col"), None),
            P(("row", "col"), None),
            P("row", "col"),
            P("row", "col"),
        ),
        out_specs=(P(None, "row", "col"), P()),
        check_vma=False,
    )
```

```python
import functools

import jax
import jax.numpy as jnp
from jax import lax
from jax.experimental import pallas as pl
from jax.experimental.pallas import tpu as pltpu
from jax.sharding import PartitionSpec as P

MESH = pl.DeviceIdType.MESH
HIGHEST = lax.Precision.HIGHEST
V, C = 256, 1024
EPS = 1e-06
NN = (((1,), (0,)), ((), ()))
NT = (((1,), (1,)), ((), ()))
TN = (((0,), (0,)), ((), ()))


def halves(a):
    hi = a.astype(jnp.bfloat16)
    return hi, (a - hi.astype(jnp.float32)).astype(jnp.bfloat16)


def left3(a, axis):
    hi, lo = halves(a)
    return jnp.concatenate([hi, lo, hi], axis=axis)


def right3(a, axis):
    hi, lo = halves(a)
    return jnp.concatenate([hi, hi, lo], axis=axis)


def dot(a, b, dims):
    return lax.dot_general(a, b, dims, preferred_element_type=jnp.float32)


def exact(a, b, dims):
    return lax.dot_general(a, b, dims, precision=HIGHEST, preferred_element_type=jnp.float32)


def kernel(
    beta_hbm, ev_hbm, q_hbm, prev_hbm, ec_hbm, pv_hbm, pc_hbm, w_hbm, b_hbm,
    out_ref,
    beta_ref, ev_ref, ec_ref, q_ref, prev_ref, own_pv, pc_other, w_ref, b_ref, pcr, pch, pcl, pv2, xg, pvc, ph, pl_,
    ap, ao, asum, aown, amps, dmine, dc, potx, pot0, ee, eo, dd, kb, r1a, r1b, acc1, r3,
    tz, txy, az, axy, mid, amid, dummy,
    load_sem, send_sem,
    x1r, x2r, x3r, p2r, p3r, p4r, cr, vr, ar_, a3r, dr, q0r, er, f1r, f3r, tr,
):
    row, col = lax.axis_index("row"), lax.axis_index("col")
    x, zhi, y = row // 8, (row // 4) % 2, row % 4
    zlo, core = col // 2, col % 2
    z = zhi * 4 + zlo
    other = 1 - core
    a, b = jnp.where(core == 0, y, x), jnp.where(core == 0, x, y)

    def dev(px, py, pz, pcore):
        return (px * 8 + (pz // 4) * 4 + py, (pz % 4) * 2 + pcore)

    def rc(src, dst, group, rs, to):
        return pltpu.make_async_remote_copy(
            src_ref=src, dst_ref=dst, send_sem=send_sem.at[group], recv_sem=rs, device_id=to, device_id_type=MESH
        )

    def px(d):
        return (x + d) % 4

    def py(d):
        return (y + d) % 4

    def pz(d):
        return (z + d) % 8

    def ab(da, db, dz=0):
        ja, jb = (a + da) % 4, (b + db) % 4
        return dev(jnp.where(core == 0, jb, ja), jnp.where(core == 0, ja, jb), pz(dz), core)

    partner = dev(x, y, z, other)

    def arrived(rs, kib):
        part = dummy.at[pl.ds(0, kib * 2)]
        rc(part, part, 0, rs, partner).wait_recv()

    def left(group, kib):
        part = dummy.at[pl.ds(0, kib * 2)]
        rc(part, part, group, x1r, partner).wait_send()

    def rows_arrived(rs, ref, n):
        part = ref.at[pl.ds(0, n)]
        rc(part, part, 0, rs, partner).wait_recv()

    def rows_left(group, ref, n):
        part = ref.at[pl.ds(0, n)]
        rc(part, part, group, x1r, partner).wait_send()

    lanes = [slice(c * 128, (c + 1) * 128) for c in range(4)]
    pairs = [(q_hbm, q_ref), (pv_hbm, own_pv)]
    for c in range(4):
        mine, its = (pl.ds(pl.multiple_of((c * 2 + k) * 128, 128), 128) for k in (core, other))
        pairs.append((pc_hbm.at[:, mine], pcr.at[zlo, core, :, lanes[c]]))
        pairs.append((pc_hbm.at[:, its], pc_other.at[:, lanes[c]]))
    pairs += [(prev_hbm, prev_ref), (ec_hbm, ec_ref), (ev_hbm, ev_ref), (beta_hbm, beta_ref)]
    pairs += [(w_hbm, w_ref), (b_hbm, b_ref)]
    loads = [pltpu.make_async_copy(s, d, load_sem.at[i]) for i, (s, d) in enumerate(pairs)]
    for c in loads:
        c.start()

    barrier = pltpu.get_barrier_semaphore()

    def greet(to):
        pl.semaphore_signal(barrier, inc=1, device_id=to, device_id_type=MESH)

    in_own_block = (x == zlo) & (core == zhi)
    own_unit = (x == 0) & (zlo == 0) & (core == zhi)
    for c in range(2):
        to = dev(zlo, y, core * 4 + (x - zlo + 4) % 4, (core + c) % 2)
        if c == 0:
            pl.when(jnp.logical_not(own_unit))(functools.partial(greet, to))
        else:
            greet(to)
    for d in range(1, 4):
        greet(dev(px(d), y, z, core))
        greet(dev(x, py(d), z, core))
    for d in (4, 3, 5, 2, 6, 1, 7):
        greet(dev(x, y, pz(d), core))
        greet(dev(x, y, pz(d), other))
    greet(partner)
    loads[0].wait()
    xg[x, zhi, y, zlo] = q_ref[0]
    for i in range(1, 10):
        loads[i].wait()

    @pl.when(own_unit)
    def _():
        pvc[y, zlo, core] = own_pv[...]
        pl.semaphore_wait(barrier, 21 + 1)

    @pl.when(jnp.logical_not(own_unit))
    def _():
        pl.semaphore_wait(barrier, 21 + 2)

    for d in (4, 3, 5, 2, 6, 1, 7):
        rc(q_ref.at[0], xg.at[x, zhi, y, zlo], 0, x1r, dev(x, y, pz(d), core)).start()

    for i in range(2):
        copy = rc(own_pv, pvc.at[y, zlo, core], 2, p2r, dev((x + zlo) % 4, y, x + 4 * ((zhi + i) % 2), zhi))
        if i == 0:
            pl.when(jnp.logical_not(own_unit))(copy.start)
        else:
            copy.start()

    def inside(s):
        return (zlo + s >= 0) & (zlo + s < 4)

    own_rows = pcr.at[zlo, core]
    rc(pc_other, own_rows, 1, cr.at[3, 1], partner).start()
    rc(own_pv, pv2.at[core], 2, vr, partner).start()
    pv2[core] = own_pv[...]
    def rows_came(s, kind):
        part = pcr.at[zlo - s, core if kind == 0 else other]
        rc(part, part, 3, cr.at[s + 3, kind], partner).wait_recv()

    arrived(x1r, 28)

    part = xg.at[x, :, y]
    for d in (2, 1, 3):
        rc(part, part, 0, x2r, ab(d, 0)).start()

    def two(wait, sem, extra=0):
        @pl.when(own_unit)
        def _():
            wait(sem, 64 + extra)

        @pl.when(jnp.logical_not(own_unit))
        def _():
            wait(sem, 128 + extra)

    two(arrived, p2r)

    def place(ja, jb):
        return jnp.where(core == 0, ja, jb), (jnp.where(core == 0, jb, ja) - zlo + 4) % 4

    def unit(da, db):
        return pvc.at[place((a + da) % 4, (b + db) % 4)]

    def p3(d):
        return rc(unit(0, 0), unit(0, 0), 5, p3r.at[d], ab(d, 0))

    def p4(d, rel):
        return rc(unit(rel, 0), unit(rel, 0), 7 if d == 2 else 6, p4r.at[d], ab(0, d))

    for d in (1, 3):
        p3(d).start()
    for s in (1, -1):

        @pl.when(inside(s))
        def _():
            rc(own_rows, own_rows, 3, cr.at[s + 3, 0], (row, (zlo + s) * 2 + core)).start()
            rc(pc_other, own_rows, 3, cr.at[s + 3, 1], (row, (zlo + s) * 2 + other)).start()

    arrived(x2r, 96)

    def chunk(c, d):
        return xg.at[px(d)] if c == 0 else xg.at[:, :, py(d)]

    for c in range(2):

        @pl.when(core == c)
        def _():
            for d in (2, 1, 3):
                rc(chunk(c, 0), chunk(c, 0), 8, x3r, ab(0, d)).start()

    def take_rows(s):
        step = 1 if s > 0 else -1

        @pl.when(inside(-s))
        def _():
            for kind in range(2):
                rows_came(s, kind)

                if abs(s) < 3:

                    @pl.when(inside(step))
                    def _():
                        part = pcr.at[zlo - s, core if kind == 0 else other]
                        rc(part, part, 9, cr.at[s + step + 3, kind], (row, (zlo + step) * 2 + core)).start()

    def pass_units():
        for d in (1, 3, 2):
            part = unit(4 - d, 0)
            rc(part, part, 5, p3r.at[d], partner).wait_recv()
            p4(1, 4 - d).start()
            p4(3, 4 - d).start()
        for rel in (3, 1, 2):
            p4(2, rel).start()

    p3(2).start()
    for d in (1, 3, 2):
        p4(d, 0).start()

    pl.when(core == 1)(pass_units)
    take_rows(1)
    take_rows(-1)
    pl.when(core == 0)(pass_units)
    arrived(x3r, 384)
    rows_came(0, 1)

    xs = left3(jnp.concatenate([xg[:, :, :, c].reshape(V, 128) for c in range(4)], axis=1), 1)

    def a1(zl):
        return rc(ap.at[zl], ao.at[zl], 10, ar_.at[zl], partner)

    def amp_of(zl):
        at = pl.ds(pl.multiple_of(zl * 128, 128), 128)
        hi, lo = halves(pcr[zl].reshape(128, 512))
        pch[at] = hi
        pcl[at] = lo
        ap[zl] = dot(jnp.concatenate([hi, hi, lo], axis=1), xs, NT).reshape(2, 64, V)
        a1(zl).start()

    amp_of(zlo)

    for s in (1, -1):
        pl.when(inside(-s))(functools.partial(amp_of, zlo - s))

    a1(zlo).wait_recv()
    asum[zlo] = ap[zlo] + ao[zlo]
    own_amp = asum[zlo]
    arrived(vr, 64)
    dens = (pv2[...] * own_amp).reshape(128, V)
    dmine[...] = exact(jnp.ones((8, V), jnp.float32), dens, NT)[0:1]
    at_end = (zlo == 0) | (zlo == 3)

    @pl.when(at_end)
    def _():
        aown[...] = asum[zlo, core]
        for c in (core, other):
            rc(aown, asum.at[zlo, core], 1, a3r, (row, (3 - zlo) * 2 + c)).start()

    slot = y * 4 + zlo
    own_row = in_own_block & (core == 0)

    def density_to(dx, dy, h):
        to = dev(px(dx), py(dy), x + 4 * ((zhi + h) % 2), zhi)
        rc(dmine, dc.at[slot], 11, dr, to).start()

    @pl.when(core == 1)
    def _():
        for i in range(24):
            density_to((2, 1, 3)[i // 8], (i // 2 + 2) % 4, i % 2)

    @pl.when(core == 0)
    def _():
        for i in range(7):
            density_to(0, (2, 2, 1, 1, 3, 3, 0)[i], (0, 1, 0, 1, 0, 1, 1)[i])

        @pl.when(own_row)
        def _():
            dc[slot] = dmine[...]

        pl.when(jnp.logical_not(own_row))(functools.partial(density_to, 0, 0, 0))

    near = zlo // 2
    far = 1 - near

    def use(zl):
        amps[pl.ds(pl.multiple_of(zl * 128, 128), 128)] = left3(asum[zl].reshape(128, V), 1)

    def join(zl):
        a1(zl).wait_recv()
        asum[zl] = ap[zl] + ao[zl]
        use(zl)

    use(zlo)
    join(near * 2 + 1 - zlo % 2)

    loads[14].wait()

    def split(d):
        hi, lo = halves(jnp.concatenate([pvc[place(j, (b + d) % 4)].reshape(128, V) for j in range(4)], axis=0))
        ph[d] = hi
        pl_[d] = lo

    def block(d, pair):
        hi, lo = ph[d], pl_[d]
        rows = pl.ds(pl.multiple_of(pair * 256, 256), 256)
        spots = [place(j, (b + d) % 4) for j in range(4)]
        columns = [pl.ds(pl.multiple_of(ys * 512 + zs * 128, 128), 128) for ys, zs in spots]
        weights = jnp.concatenate([w_ref[rows, at] for at in columns], axis=1)
        terms = dot(amps[rows], jnp.concatenate([hi, hi, lo], axis=1), NT) * weights
        return dot(left3(terms, 1), jnp.concatenate([hi, hi, lo], axis=0), NN)

    def e1(i, pair):
        part = pl.ds(2 * pair, 2)
        return rc(ee.at[part], eo.at[part], 13, er.at[i], partner)

    split(0)
    part = block(0, near)
    take_rows(2)
    take_rows(-2)
    for s in (2, -2):
        pl.when(inside(-s))(functools.partial(amp_of, zlo - s))

    arrived(p4r.at[1], 512)
    split(3)
    part = part + block(3, near)
    arrived(p4r.at[3], 512)
    split(1)
    part = part + block(1, near)
    ee[pl.ds(2 * near, 2)] = part.reshape(2, 2, 64, V)
    arrived(p4r.at[2], 512)
    split(2)
    ee[pl.ds(2 * near, 2)] += block(2, near).reshape(2, 2, 64, V)
    e1(0, near).start()

    loads[15].wait()

    @pl.when(own_row)
    def _():
        rows_arrived(dr, dc, 15)

    @pl.when(jnp.logical_not(own_row))
    def _():
        rows_arrived(dr, dc, 16)

    pot = None
    for t in range(16):
        piece = b_ref[:, t * 128 : (t + 1) * 128] * dc[t]
        pot = piece if pot is None else pot + piece
    pot = jnp.sum(pot, axis=1, keepdims=True)
    diag = lax.broadcasted_iota(jnp.int32, (128, 128), 0) == lax.broadcasted_iota(jnp.int32, (128, 128), 1)
    for j in range(4):
        potx[j] = jnp.sum(jnp.where(diag, pot[j * 128 : (j + 1) * 128], 0.0), axis=0, keepdims=True)
    for d in (2, 1, 3, 0):
        zl = (zlo + d) % 4
        for c in range(2):
            if d or c:
                rc(potx.at[zl], pot0.at[2 * d + c], 15, q0r, (row, zl * 2 + (core + c) % 2)).start()
    pot0[0] = potx[zlo]
    for s in (2, -2):
        pl.when(inside(-s))(functools.partial(join, zlo - s))

    @pl.when(at_end)
    def _():
        arrived(a3r, 128)
        use(3 - zlo)

    @pl.when(jnp.logical_not(at_end))
    def _():
        join(3 - zlo)

    part = block(0, far) + block(3, far) + block(1, far) + block(2, far)
    ee[pl.ds(2 * far, 2)] = part.reshape(2, 2, 64, V)
    e1(1, far).start()

    for s in (3, -3):
        take_rows(s)

        @pl.when(inside(-s))
        def _():
            at = pl.ds(pl.multiple_of((zlo - s) * 128, 128), 128)
            hi, lo = halves(pcr[zlo - s].reshape(128, 512))
            pch[at] = hi
            pcl[at] = lo

    def kpart(i, pair):
        e1(i, pair).wait_recv()
        at = pl.ds(2 * pair, 2)
        both = -(ee[at] + eo[at])
        dd[at] = both
        rows = pl.ds(pl.multiple_of(pair * 256, 256), 256)
        hi, lo = pch[rows], pcl[rows]
        return dot(left3(both.reshape(256, V), 0), jnp.concatenate([hi, hi, lo], axis=0), TN)

    kfull = kpart(0, near)
    kfull = kfull + kpart(1, far)
    rows_arrived(q0r, pot0, 7)
    pot_row = jnp.sum(pot0[...], axis=0)
    pot2 = 2.0 * jnp.sum(jnp.where(diag, pot_row, 0.0), axis=1, keepdims=True)
    bare = pot2 * pv2[...].reshape(128, V)
    rows = pl.ds(pl.multiple_of(zlo * 128, 128), 128)
    hi, lo = pch[rows], pcl[rows]
    kfull = kfull + dot(left3(bare, 0), jnp.concatenate([hi, hi, lo], axis=0), TN)
    dd[zlo] = dd[zlo] + bare.reshape(2, 64, V)
    for c in range(4):
        kb[:, :, :, c] = kfull[:, lanes[c]].reshape(4, 2, 4, 8, 128)

    for c in range(2):

        @pl.when(core == c)
        def _():
            for d in (2, 1, 3):
                part = kb.at[px(d)] if c == 0 else kb.at[:, :, py(d)]
                rc(part, (r1a if c == 0 else r1b).at[d - 1], 16, f1r, ab(0, d)).start()

    for i in (10, 11, 12, 13):
        loads[i].wait()
    q, prev = q_ref[0], prev_ref[0]
    sub8 = lax.broadcasted_iota(jnp.int32, (8, 128), 0)
    ev = jnp.zeros((8, 128), jnp.float32)
    for i in range(8):
        ev = jnp.where(sub8 == i, ev_ref[i], ev)
    gaps = ec_ref[...].reshape(1, 128) - ev
    prod = (dd[:, core] * asum[:, core]).reshape(256, V)
    prod = jnp.sum(prod[:, 0:128] + prod[:, 128:256], axis=0, keepdims=True)
    qq = jnp.sum(q * q, axis=0, keepdims=True)
    qu = prod + jnp.sum(gaps * q * q, axis=0, keepdims=True)
    az[0] = jnp.concatenate([qu, qq], axis=1)

    def t1(src, dst, group, rs):
        for d in (4, 3, 5, 2, 6, 1, 7, 0):
            for j in (d, d + 8):
                if j:
                    to = dev(x, y, pz(d), core if j < 8 else other)
                    rc(src, dst.at[j], group, rs, to).start()

    def t2(src, dst, group, rs):
        for j in (10, 9, 11, 6, 14, 2, 8, 5, 7, 13, 15, 1, 3, 4, 12):
            rc(src, dst.at[j], group, rs, dev(px(j // 4), py(j % 4), z, core)).start()

    t1(az.at[0], az, 18, tr.at[0])

    arrived(f1r, 384)
    for c in range(2):

        @pl.when(core == c)
        def _():
            if c == 0:
                for i in range(2):
                    acc1[:, i] = kb[x, i] + r1a[0, i] + r1a[1, i] + r1a[2, i]
            else:
                acc1[...] = kb[:, :, y] + r1b[0] + r1b[1] + r1b[2]

    for da in (2, 1, 3, 0):
        for dz in (4, 3, 5, 2, 6, 1, 7, 0):
            if da or dz:
                zz = pz(dz)
                part = acc1.at[(a + da) % 4, zz // 4, zz % 4]
                rc(part, r3.at[da * 8 + dz], 17, f3r, ab(da, 0, dz)).start()
    rows_arrived(tr.at[0], az, 15)
    amid[...] = jnp.sum(az[...], axis=0)
    axy[0] = amid[...]
    t2(amid, axy, 19, tr.at[1])
    arrived(f3r, 124)
    tile = acc1[a, zhi, zlo] + jnp.sum(r3[1:32], axis=0)
    inv = 1.0 / (V * C)
    bp = beta_ref[...]
    rows_arrived(tr.at[1], axy, 15)
    total = jnp.sum(axy[...], axis=0)
    qu = jnp.sum(total[:, 0:128], axis=1, keepdims=True)
    qq = jnp.sum(total[:, 128:256], axis=1, keepdims=True)
    alpha = qu * inv / (qq * inv + EPS)
    resid = tile + (gaps - alpha) * q - bp * prev
    tz[0] = jnp.sum(resid * resid, axis=0, keepdims=True)
    t1(tz.at[0], tz, 20, tr.at[2])
    rows_arrived(tr.at[2], tz, 15)
    mid[...] = jnp.sum(tz[...], axis=0)
    t2(mid, txy, 21, tr.at[3])
    txy[0] = mid[...]
    rows_arrived(tr.at[3], txy, 15)
    ww = jnp.sum(jnp.sum(txy[...], axis=0), axis=1, keepdims=True)
    beta = jnp.sqrt(ww * inv + EPS)
    out_ref[0:8] = resid / beta
    out_ref[8:16] = jnp.where(lax.broadcasted_iota(jnp.int32, (8, 128), 1) == 0, alpha, beta)

    left(0, 124)
    two(left, 2, 64)
    left(5, 384)
    left(6, 1024)
    left(7, 512)
    left(8, 384)

    @pl.when((zlo == 0) | (zlo == 3))
    def _():
        left(1, 256)
        left(3, 256)
        left(10, 384)

    @pl.when((zlo == 1) | (zlo == 2))
    def _():
        left(1, 128)
        left(3, 512)
        left(9, 768)
        left(10, 512)


    @pl.when(core == 1)
    def _():
        left(11, 12)

    @pl.when(core == 0)
    def _():
        pl.when(own_row)(lambda: rows_left(11, dc, 7))
        pl.when(jnp.logical_not(own_row))(lambda: rows_left(11, dc, 8))

    left(13, 512)
    rows_left(15, pot0, 7)
    left(16, 384)
    left(17, 124)
    rows_left(18, az, 15)
    rows_left(19, axy, 15)
    rows_left(20, tz, 15)
    rows_left(21, txy, 15)


def split_results(both_ref, out_ref, coef_ref):
    out_ref[0] = both_ref[0:8]
    coef_ref[...] = both_ref[8:9, 0:2]


def per_device(q, prev, beta, ev, ec, pv, pc, w, b):
    f32 = jnp.float32
    vmem = pl.BlockSpec(memory_space=pltpu.VMEM)
    hbm = pl.BlockSpec(memory_space=pltpu.HBM)

    def buf(*shape):
        return pltpu.VMEM(shape, f32)

    def sem(*n):
        return pltpu.SemaphoreType.DMA(n)

    tile = (8, 128)
    bf16 = jnp.bfloat16
    scratch = [
        buf(1, 1), pltpu.SMEM((8,), f32), buf(128),
        buf(1, *tile), buf(1, *tile), buf(64, V), buf(64, 512), buf(512, 2048), buf(512, 2048),
        buf(4, 2, 64, 512), pltpu.VMEM((512, 512), bf16), pltpu.VMEM((512, 512), bf16), buf(2, 64, V),
        buf(4, 2, 4, 4, *tile), buf(4, 4, 2, 64, V), pltpu.VMEM((4, 512, V), bf16), pltpu.VMEM((4, 512, V), bf16),
        buf(4, 2, 64, V), buf(4, 2, 64, V), buf(4, 2, 64, V), buf(64, V), pltpu.VMEM((512, 3 * V), bf16),
        buf(1, 128), buf(16, 1, 128), buf(4, 1, 128), buf(8, 1, 128),
        buf(4, 2, 64, V), buf(4, 2, 64, V), buf(4, 2, 64, V),
        buf(4, 2, 4, 4, *tile), buf(3, 2, 4, 4, *tile), buf(3, 4, 2, 4, *tile), buf(4, 2, 4, *tile), buf(32, *tile),
        buf(16, 1, 128), buf(16, 1, 128), buf(16, 1, 256), buf(16, 1, 256), buf(1, 128), buf(1, 256), buf(2048, 128),
        sem(16), sem(22),
        sem(), sem(), sem(), sem(), sem(4), sem(4), sem(7, 2), sem(), sem(4), sem(), sem(), sem(),
        sem(2), sem(), sem(), sem(4),
    ]
    both = pl.pallas_call(
        kernel,
        out_shape=jax.ShapeDtypeStruct((16, 128), f32),
        in_specs=[hbm] * 9,
        out_specs=vmem,
        scratch_shapes=scratch,
        compiler_params=pltpu.CompilerParams(
            collective_id=0, has_side_effects=True, vmem_limit_bytes=60 * 1024 * 1024
        ),
        name="lanczos_step",
    )(beta.reshape(1, 1), ev, q, prev, ec, pv, pc, w, b)
    return pl.pallas_call(
        split_results,
        out_shape=(jax.ShapeDtypeStruct((1, 8, 128), f32), jax.ShapeDtypeStruct((1, 2), f32)),
        in_specs=[vmem],
        out_specs=(vmem, vmem),
        name="split_results",
    )(both)


def solution(mesh):
    return jax.shard_map(
        per_device,
        mesh=mesh,
        in_specs=(
            P(None, "row", "col"),
            P(None, "row", "col"),
            P(),
            P("row"),
            P("col"),
            P(("row", "col"), None),
            P(("row", "col"), None),
            P("row", "col"),
            P("row", "col"),
        ),
        out_specs=(P(None, "row", "col"), P()),
        check_vma=False,
    )
```
